32 devices in a mesh: rep: 4 (over y, x), grp: 8 (over z, core).
Axes of the slice: x: 2, y: 2, z: 4, core: 2. Of those that a mesh axis runs over, the one named last changes fastest.
Arguments:
- block_in: bfloat16 [18912, 768], P(('rep', 'grp')), may hold values from -26 to 26
- out_grad: bfloat16 [18912, 768], P(('rep', 'grp')), may hold values from -6 to 6
- routes: int32 [18912, 2], P(('rep', 'grp')), may hold values from 0 to 31, all different within a row; in each aligned block of 591 rows (0 to 590, 591 to 1181, ...) at most 73 rows name the same one
- ln1_gain: bfloat16 [768], P('grp'), may hold values from 0.5 to 1.5
- ln1_bias: bfloat16 [768], P('grp'), may hold values from -3 to 3
- w_qkv: bfloat16 [768, 2304], P('grp'), may hold values from -0.21875 to 0.21875
- w_proj: bfloat16 [768, 768], P('grp'), may hold values from -0.625 to 0.625
- ln2_gain: bfloat16 [768], P('grp'), may hold values from 0.5 to 1.5
- ln2_bias: bfloat16 [768], P('grp'), may hold values from -3 to 3
- w_fc1: bfloat16 [768, 3072], P('grp'), may hold values from -0.21875 to 0.21875
- w_fc2: bfloat16 [3072, 768], P('grp'), may hold values from -0.109375 to 0.109375
- ln3_gain: bfloat16 [768], P('grp'), may hold values from 0.5 to 1.5
- ln3_bias: bfloat16 [768], P('grp'), may hold values from -3 to 3
- w_router: bfloat16 [768, 32], P('grp'), may hold values from -1 to 1
- expert_in: bfloat16 [32, 768, 3072], P('grp'), may hold values from -0.21875 to 0.21875
- expert_out: bfloat16 [32, 3072, 768], P('grp'), may hold values from -0.109375 to 0.109375
Outputs:
- block_out: float32 [18912, 768], P(('rep', 'grp'))
- grad_in: float32 [18912, 768], P(('rep', 'grp'))
- grad_ln1_gain: float32 [768], P('grp')
- grad_ln1_bias: float32 [768], P('grp')
- grad_qkv: float32 [768, 2304], P('grp')
- grad_proj: float32 [768, 768], P('grp')
- grad_ln2_gain: float32 [768], P('grp')
- grad_ln2_bias: float32 [768], P('grp')
- grad_fc1: float32 [768, 3072], P('grp')
- grad_fc2: float32 [3072, 768], P('grp')
- grad_ln3_gain: float32 [768], P('grp')
- grad_ln3_bias: float32 [768], P('grp')
- grad_router: float32 [768, 32], P('grp')
- grad_expert_in: float32 [32, 768, 3072], P('grp')
- grad_expert_out: float32 [32, 3072, 768], P('grp')
The draws below stay inside these ranges and needn't reach their ends.
Inputs may be any that keep to these rules, and one draw needn't show every extreme that they name: `routes`: in each aligned block of 591 rows (the tokens of one device) no expert is named by more than 73 rows, a bound that some block reaches; the two experts of a row differ; every expert is named somewhere.
All inputs are finite; a program needn't handle non-finite values.
Results may differ from the reference program's by a relative error of at most 0.02.
Values may be sent and summed in bfloat16 or wider, within the bound.
A program may use at most 384 MiB of HBM per device.

```python
import math
import jax
import jax.numpy as jnp
import numpy as np
from jax import lax

D = 768
HEADS = 12
HEAD_DIM = 64
FF = 3072
EXPERTS = 32
SEQ_LEN = 197
TOK_DEV = 591
CAP = 73
SEQS = 96
TOKENS = 18912
N_REP = 4
N_GRP = 8


def draw_block_in(key, part):
    first, second, third = jax.random.split(key, 3)
    row_scale = jnp.exp(jax.random.uniform(first, (TOKENS, 1), jnp.float32, math.log(0.316), math.log(3.16)))
    col_scale = jnp.exp(jax.random.uniform(second, (1, D), jnp.float32, math.log(0.5), math.log(2.0)))
    base_draw = jnp.clip(jax.random.normal(third, (TOKENS, D), jnp.float32), -4.0, 4.0)
    return (base_draw * row_scale * col_scale).astype(jnp.bfloat16)


def draw_w_router(key, part):
    base_draw = jnp.clip(jax.random.normal(key, (D, EXPERTS), jnp.float32), -3.0, 3.0) * 3.0 * D ** (-0.5)
    return base_draw.astype(jnp.bfloat16)


def block_levels(stream_key, extent, cuts, low, top_value):
    loudness = 1.0
    for dim, blocks in cuts:
        steps = jax.random.uniform(jax.random.fold_in(jax.random.fold_in(stream_key, 6), dim), (blocks,), jnp.float32, low / len(cuts), top_value / len(cuts))
        loudness = loudness * jnp.repeat(jnp.exp(steps), extent[dim] // blocks).reshape((-1,) + (1,) * (len(extent) - 1 - dim))
    return loudness


def shared_out(own_key, own, number, rows, number_of, top, most, skew):
    sequence = jax.random.permutation(own_key, number_of)
    crowded, usual = load_shares(number_of, rows * top, most, skew, True), load_shares(number_of, rows * top, most, skew, False)
    places = jnp.arange(number_of)

    def named(tallies, turn):
        used = int((tallies > 0).sum())
        fixed = max(1, used // 4)
        passed = fixed + (places - fixed + turn * (used - fixed)) % max(1, number_of - fixed)
        return jnp.zeros((number_of,), jnp.int32).at[sequence[jnp.where(places < fixed, places, passed)]].set(jnp.asarray(tallies, jnp.int32))

    tallies = jnp.where(number % 4 == 0, named(crowded, number // 4), named(usual, number - number // 4 - 1))
    mixed = jax.random.permutation(jax.random.fold_in(own, 3), number_of)
    source_of, taker = mixed[0:number_of // 2 * 2:2], mixed[1:number_of // 2 * 2:2]
    room = jnp.minimum(tallies[source_of] - 1, most - tallies[taker]) // 2
    room = jnp.where((source_of == sequence[0]) | (taker == sequence[0]) | (tallies[taker] == 0), 0, jnp.maximum(room, 0))
    passed = jax.random.randint(jax.random.fold_in(own, 4), (number_of // 2,), 0, 1 << 20) % (room + 1)
    tallies = tallies.at[source_of].add(-passed).at[taker].add(passed)
    labels = jnp.searchsorted(jnp.cumsum(tallies), jnp.arange(rows * top), side="right").astype(jnp.int32)
    grid = labels.reshape(top, rows).T
    grid = grid[jax.random.permutation(jax.random.fold_in(own, 1), rows)]
    turn = jax.random.randint(jax.random.fold_in(own, 2), (rows, 1), 0, top)
    return jnp.take_along_axis(grid, (jnp.arange(top)[None, :] + turn) % top, axis=1)


def load_shares(number_of, total, most, skew, full):
    weights = [(1 << 20) // math.isqrt(standing ** skew) + 1 for standing in range(1, number_of + 1)]
    largest = most if full else min(most, max(-(-total // number_of), total * weights[0] // sum(weights)))
    least = 1 if total - largest >= number_of - 1 else 0
    given, surplus = [largest] + [least] * (number_of - 1), total - largest - least * (number_of - 1)
    while surplus > 0:
        free = [i for i in range(1, number_of) if given[i] < largest] or [i for i in range(1, number_of) if given[i] < most]
        pool, budget = sum([weights[i] for i in free]), surplus
        for i in free:
            more = min(most - given[i], max(1, budget * weights[i] // pool), surplus)
            given[i] = given[i] + more
            surplus = surplus - more
    return np.array(given)


def centred(key, shape, deviation, reach, cuts=(), kind=jnp.bfloat16):
    loudness = block_levels(key, shape, cuts, -0.22, 0.18) if cuts else 1.0
    drawn = jax.random.normal(key, shape, jnp.float32) * deviation * loudness
    return jnp.minimum(jnp.maximum(drawn, -reach), reach).astype(kind)


def setup_inputs(seed: int = 0) -> dict:
    key_of = jax.random.split(jax.random.key(seed), 17)
    block_in = draw_block_in(jax.random.fold_in(key_of[16], 71), 0)
    out_grad = centred(key_of[1], (TOKENS, D), 1.0, 6.0, ((0, 32),))
    routes_keys = jax.random.split(jax.random.fold_in(key_of[2], 1), TOKENS // TOK_DEV)
    routes_turns = jax.random.permutation(jax.random.fold_in(key_of[2], 3), TOKENS // TOK_DEV)
    routes = jax.vmap(lambda own, number: shared_out(jax.random.fold_in(key_of[2], 2), own, number, TOK_DEV, EXPERTS, 2, CAP, 1))(routes_keys, routes_turns).reshape((TOKENS, 2))
    ln1_gain = jnp.clip(1.0 + 0.1 * jax.random.normal(key_of[3], (D,), jnp.float32), 0.5, 1.5).astype(jnp.bfloat16)
    ln1_bias = centred(key_of[4], (D,), 0.3, 3.0, ((0, 8),))
    w_qkv = centred(key_of[5], (D, 3 * D), D ** -0.5, 0.21875, ((0, 8),))
    w_proj = centred(key_of[6], (D, D), (D // 8) ** -0.5, 0.625, ((0, 8),))
    ln2_gain = jnp.clip(1.0 + 0.1 * jax.random.normal(key_of[7], (D,), jnp.float32), 0.5, 1.5).astype(jnp.bfloat16)
    ln2_bias = centred(key_of[8], (D,), 0.3, 3.0, ((0, 8),))
    w_fc1 = centred(key_of[9], (D, FF), D ** -0.5, 0.21875, ((0, 8),))
    w_fc2 = centred(key_of[10], (FF, D), FF ** -0.5, 0.109375, ((0, 8),))
    ln3_gain = jnp.clip(1.0 + 0.1 * jax.random.normal(key_of[11], (D,), jnp.float32), 0.5, 1.5).astype(jnp.bfloat16)
    ln3_bias = centred(key_of[12], (D,), 0.3, 3.0, ((0, 8),))
    w_router = draw_w_router(jax.random.fold_in(key_of[16], 71), 0)
    expert_in = centred(key_of[14], (EXPERTS, D, FF), D ** -0.5, 0.21875, ((0, 8),))
    expert_out = centred(key_of[15], (EXPERTS, FF, D), FF ** -0.5, 0.109375, ((0, 8),))
    return dict(block_in=block_in, out_grad=out_grad, routes=routes, ln1_gain=ln1_gain, ln1_bias=ln1_bias, w_qkv=w_qkv, w_proj=w_proj, ln2_gain=ln2_gain, ln2_bias=ln2_bias, w_fc1=w_fc1, w_fc2=w_fc2, ln3_gain=ln3_gain, ln3_bias=ln3_bias, w_router=w_router, expert_in=expert_in, expert_out=expert_out)


@jax.custom_vjp
def low(v):
    return lax.optimization_barrier(v.astype(jnp.bfloat16)).astype(jnp.float32)

@jax.custom_vjp
def low_back(v):
    return v

def low_keep(v):
    return (low(v), None)

def low_pass(kept, grad):
    return (grad,)

def back_keep(v):
    return (v, None)

def back_low(kept, grad):
    return (low(grad),)
low.defvjp(low_keep, low_pass)
low_back.defvjp(back_keep, back_low)

def matmul(left_side, right_side):
    return jnp.dot(left_side, right_side, precision=lax.Precision.HIGHEST, preferred_element_type=jnp.float32)

def layer_norm(operand, norm_gain, norm_shift):
    row_mean = lax.optimization_barrier(jnp.mean(operand, axis=-1, keepdims=True))
    center = operand - row_mean
    spread = lax.optimization_barrier(jnp.mean(center * center, axis=-1, keepdims=True))
    return center * lax.rsqrt(spread + 1e-06) * norm_gain + norm_shift

def dense_block(rows, dense_params):
    gain_one, shift_one, w_qkv, w_proj, gain_two, shift_two, w_fc1, w_fc2 = dense_params
    seq_count = rows.shape[0] // SEQ_LEN
    normed = low(layer_norm(rows, gain_one, shift_one))
    packed = low(low_back(matmul(normed, w_qkv)))
    split_heads = packed.reshape(seq_count, SEQ_LEN, 3, HEADS, HEAD_DIM)
    raw_scores = jnp.einsum('bqhd,bkhd->bhqk', split_heads[:, :, 0], split_heads[:, :, 1], precision=lax.Precision.HIGHEST)
    scores = low_back(raw_scores * HEAD_DIM ** (-0.5))
    softmaxed = low(jax.nn.softmax(scores, axis=-1))
    attn_mixed = jnp.einsum('bhqk,bkhd->bqhd', softmaxed, split_heads[:, :, 2], precision=lax.Precision.HIGHEST)
    attn_mixed = low(low_back(attn_mixed.reshape(rows.shape[0], HEADS * HEAD_DIM)))
    attended = rows + low_back(matmul(attn_mixed, w_proj))
    normed_two = low(layer_norm(attended, gain_two, shift_two))
    hidden = low(jax.nn.gelu(low_back(matmul(normed_two, w_fc1)), approximate=False))
    return attended + low_back(matmul(hidden, w_fc2))

def expert_rows(normed, weights):
    weight_in, weight_out, slot_rows = weights
    sent_rows = low_back(normed[slot_rows // 2])
    expert_inner = low_back(matmul(sent_rows, weight_in))
    expert_act = low(jax.nn.gelu(expert_inner, approximate=False))
    return low(low_back(matmul(expert_act, weight_out)))

def reference(block_in, out_grad, routes, ln1_gain, ln1_bias, w_qkv, w_proj, ln2_gain, ln2_bias, w_fc1, w_fc2, ln3_gain, ln3_bias, w_router, expert_in, expert_out):
    flat_routes = routes.reshape(-1)
    total_slots = CAP * N_REP * N_GRP

    def pick_rows(expert):
        sorted_rows = jnp.argsort((flat_routes != expert).astype(jnp.int32), stable=True)[:total_slots]
        return sorted_rows.astype(jnp.int32)
    expert_ids = jnp.arange(EXPERTS, dtype=jnp.int32)
    slot_rows = jax.vmap(pick_rows)(expert_ids)
    filled = flat_routes[slot_rows] == expert_ids[:, None]
    seq_group = math.gcd(SEQS, 16)

    def forward(inputs, dense_params, expert_params):

        def dense_run(rows):
            return dense_block(rows, dense_params)
        grouped = inputs.reshape(SEQS // seq_group, seq_group * SEQ_LEN, D)
        second = lax.map(jax.checkpoint(dense_run), grouped).reshape(TOKENS, D)
        gain_three, shift_three, weight_router, weight_in, weight_out = expert_params
        normed = low(layer_norm(second, gain_three, shift_three))
        logits = matmul(normed, weight_router)
        gate_probs = jax.nn.softmax(jnp.take_along_axis(logits, routes, axis=1), axis=-1)

        def run_expert(weights):
            return expert_rows(normed, weights)
        produced = lax.map(jax.checkpoint(run_expert), (weight_in, weight_out, slot_rows))
        slot_gates = jnp.where(filled, gate_probs.reshape(-1)[slot_rows], 0.0)
        scaled = produced * slot_gates[:, :, None]
        combined = jnp.zeros((TOKENS, D), jnp.float32).at[(slot_rows // 2).reshape(-1)].add(scaled.reshape(-1, D))
        return second + combined
    dense_params = (ln1_gain.astype(jnp.float32), ln1_bias.astype(jnp.float32), w_qkv.astype(jnp.float32), w_proj.astype(jnp.float32), ln2_gain.astype(jnp.float32), ln2_bias.astype(jnp.float32), w_fc1.astype(jnp.float32), w_fc2.astype(jnp.float32))
    expert_params = (ln3_gain.astype(jnp.float32), ln3_bias.astype(jnp.float32), w_router.astype(jnp.float32), expert_in.astype(jnp.float32), expert_out.astype(jnp.float32))
    result, pullback = jax.vjp(forward, block_in.astype(jnp.float32), dense_params, expert_params)
    grad_in, grad_dense, grad_expert = pullback(out_grad.astype(jnp.float32))
    grad_ln1_gain, grad_ln1_bias, grad_qkv, grad_proj, grad_ln2_gain, grad_ln2_bias, grad_fc1, grad_fc2 = grad_dense
    grad_ln3_gain, grad_ln3_bias, grad_router, grad_expert_in, grad_expert_out = grad_expert
    return (result, grad_in, grad_ln1_gain, grad_ln1_bias, grad_qkv, grad_proj, grad_ln2_gain, grad_ln2_bias, grad_fc1, grad_fc2, grad_ln3_gain, grad_ln3_bias, grad_router, grad_expert_in, grad_expert_out)
```

```python
import functools

import jax
import jax.numpy as jnp
from jax import lax
from jax.sharding import PartitionSpec as P

HEADS = 12
HEAD_DIM = 64
EXPERTS = 32
SEQ_LEN = 197
CAP = 73
SLOTS = 80


def layer_norm(operand, norm_gain, norm_shift):
    row_mean = jnp.mean(operand, axis=-1, keepdims=True)
    center = operand - row_mean
    spread = jnp.mean(center * center, axis=-1, keepdims=True)
    return center * lax.rsqrt(spread + 1e-06) * norm_gain + norm_shift


def gelu_pair(x):
    falling = jnp.exp(-0.5 * x * x)
    t = 1.0 / (1.0 + (0.3275911 * 0.7071067811865476) * jnp.abs(x))
    series = 0.5 * 1.061405429
    for coefficient in (-1.453152027, 1.421413741, -0.284496736, 0.254829592):
        series = series * t + 0.5 * coefficient
    beyond = series * t * falling
    below = jnp.where(x < 0, beyond, 1.0 - beyond)
    return x * below, below + x * (falling * 0.3989422804014327)


def norm_back(operand, norm_gain, norm_shift, upstream):
    result, pullback = jax.vjp(layer_norm, operand, norm_gain, norm_shift)
    return pullback(upstream)


def dense_product(left_side, right_side):
    return jnp.dot(left_side, right_side, preferred_element_type=jnp.float32)


def rows_product(left_side, right_side):
    return lax.dot_general(
        left_side, right_side, (((0,), (0,)), ((), ())), preferred_element_type=jnp.float32
    )


def column_product(left_side, right_side):
    return lax.dot_general(
        left_side, right_side, (((1,), (1,)), ((), ())), preferred_element_type=jnp.float32
    )


def attend(packed, scaling):
    seq_count = packed.shape[0] // SEQ_LEN
    split_heads = packed.reshape(seq_count, SEQ_LEN, 3, HEADS, HEAD_DIM)
    scores = (
        jnp.einsum(
            "bqhd,bkhd->bhqk",
            split_heads[:, :, 0],
            split_heads[:, :, 1],
            preferred_element_type=jnp.float32,
        )
        * scaling
    )
    row_top = jnp.max(scores, axis=-1, keepdims=True)
    exp_scores = jnp.exp(scores - row_top)
    row_total = jnp.sum(exp_scores, axis=-1, keepdims=True)
    softmaxed = (exp_scores / row_total).astype(jnp.bfloat16)
    attn_mixed = jnp.einsum(
        "bhqk,bkhd->bqhd", softmaxed, split_heads[:, :, 2], preferred_element_type=jnp.float32
    )
    return (
        attn_mixed.reshape(packed.shape[0], HEADS * HEAD_DIM).astype(jnp.bfloat16),
        row_top + jnp.log(row_total),
    )


def attend_back(packed, log_total, grad_mixed, scaling):
    seq_count = packed.shape[0] // SEQ_LEN
    split_heads = packed.reshape(seq_count, SEQ_LEN, 3, HEADS, HEAD_DIM)
    queries = split_heads[:, :, 0]
    key_rows = split_heads[:, :, 1]
    value_rows = split_heads[:, :, 2]
    scores = (
        jnp.einsum("bqhd,bkhd->bhqk", queries, key_rows, preferred_element_type=jnp.float32)
        * scaling
    )
    softmaxed = jnp.exp(scores - log_total)
    grad_heads = grad_mixed.reshape(seq_count, SEQ_LEN, HEADS, HEAD_DIM)
    grad_probs = jnp.einsum(
        "bqhd,bkhd->bhqk", grad_heads, value_rows, preferred_element_type=jnp.float32
    )
    grad_values = jnp.einsum(
        "bhqk,bqhd->bkhd",
        softmaxed.astype(jnp.bfloat16),
        grad_heads,
        preferred_element_type=jnp.float32,
    )
    row_inner = jnp.sum(grad_probs * softmaxed, axis=-1, keepdims=True)
    grad_scores = (softmaxed * (grad_probs - row_inner)).astype(jnp.bfloat16)
    grad_queries = (
        jnp.einsum("bhqk,bkhd->bqhd", grad_scores, key_rows, preferred_element_type=jnp.float32)
        * scaling
    )
    grad_keys = (
        jnp.einsum("bhqk,bqhd->bkhd", grad_scores, queries, preferred_element_type=jnp.float32)
        * scaling
    )
    stacked = jnp.stack([grad_queries, grad_keys, grad_values], axis=2)
    return stacked.reshape(packed.shape[0], 3 * HEADS * HEAD_DIM).astype(jnp.bfloat16)


def swap(operand, axis_pairs):
    return lax.ppermute(operand, "rep", axis_pairs)


def local(
    n_rep,
    n_grp,
    block_in,
    out_grad,
    routes,
    ln1_gain,
    ln1_bias,
    w_qkv,
    w_proj,
    ln2_gain,
    ln2_bias,
    w_fc1,
    w_fc2,
    ln3_gain,
    ln3_bias,
    w_router,
    expert_in,
    expert_out,
):
    bf16, f32 = jnp.bfloat16, jnp.float32
    scaling = HEAD_DIM ** (-0.5)
    tok_rows, width = block_in.shape
    held = expert_in.shape[0]
    spread = n_rep if held % n_rep == 0 else 1
    own = held // spread
    axes = ("rep", "grp") if spread > 1 else ("grp",)
    peers = spread * n_grp
    rep_at = lax.axis_index("rep")

    def gather(shard):
        return lax.all_gather(shard, "grp", axis=0, tiled=True)

    small = gather(jnp.stack([ln1_gain, ln1_bias, ln2_gain, ln2_bias, ln3_gain, ln3_bias], axis=1))
    full_qkv = gather(w_qkv)
    full_proj = gather(w_proj)
    full_fc1 = gather(w_fc1)
    full_fc2 = gather(w_fc2)
    full_router = gather(w_router)
    small = small.astype(f32).T
    gain_first, shift_first, gain_second, shift_second, gain_third, shift_third = small

    expert_ids = lax.iota(jnp.int32, EXPERTS)
    route_picks = routes[:, :, None] == expert_ids[None, None, :]
    hits = jnp.any(route_picks, axis=1)
    earlier = (
        lax.broadcasted_iota(jnp.int32, (tok_rows, tok_rows), 1)
        < lax.broadcasted_iota(jnp.int32, (tok_rows, tok_rows), 0)
    ).astype(bf16)
    ranks = dense_product(earlier, hits.astype(bf16)).astype(jnp.int32)
    rank = jnp.sum(jnp.where(route_picks, ranks[:, None, :], 0), axis=-1)
    group_of, within = routes // held, routes % held
    place = ((within // own) * n_grp + group_of) * own + within % own
    slot = place * SLOTS + rank
    slot_ids = lax.iota(jnp.int32, EXPERTS * SLOTS)
    pick_first = (slot[:, 0][:, None] == slot_ids[None, :]).astype(bf16)
    pick_second = (slot[:, 1][:, None] == slot_ids[None, :]).astype(bf16)
    pick_both = pick_first + pick_second

    def exchange(rows):
        return lax.all_to_all(rows, axes, split_axis=0, concat_axis=0, tiled=True)

    def to_experts(rows):
        rows = rows.reshape((peers, own, SLOTS) + rows.shape[1:])
        return jnp.moveaxis(exchange(rows), 1, 0).reshape((own, peers * SLOTS) + rows.shape[3:])

    def to_tokens(rows):
        rows = jnp.moveaxis(rows.reshape((own, peers, SLOTS) + rows.shape[2:]), 1, 0)
        return exchange(rows).reshape((EXPERTS * SLOTS,) + rows.shape[3:])

    grad_slots = to_experts(rows_product(pick_both, out_grad).astype(bf16))

    stream = block_in.astype(f32)
    normed_one = layer_norm(stream, gain_first, shift_first).astype(bf16)
    packed = dense_product(normed_one, full_qkv).astype(bf16)
    attn_mixed, log_total = attend(packed, scaling)
    after_attn = stream + dense_product(attn_mixed, full_proj)
    normed_two = layer_norm(after_attn, gain_second, shift_second).astype(bf16)
    hidden, hidden_slope = gelu_pair(dense_product(normed_two, full_fc1))
    hidden, hidden_slope = hidden.astype(bf16), hidden_slope.astype(bf16)
    second = after_attn + dense_product(hidden, full_fc2)
    normed_three = layer_norm(second, gain_third, shift_third).astype(bf16)
    arrived = to_experts(rows_product(pick_both, normed_three).astype(bf16))

    logits = dense_product(normed_three, full_router)
    chosen = jnp.sum(jnp.where(route_picks, logits[:, None, :], 0.0), axis=-1)
    chosen_exp = jnp.exp(chosen - jnp.max(chosen, axis=-1, keepdims=True))
    gate_probs = chosen_exp / jnp.sum(chosen_exp, axis=-1, keepdims=True)
    hit_first = slot[:, 0][:, None] == slot_ids[None, :]
    hit_second = slot[:, 1][:, None] == slot_ids[None, :]
    gate_rows = jnp.sum(
        jnp.where(hit_first, gate_probs[:, 0][:, None], 0.0)
        + jnp.where(hit_second, gate_probs[:, 1][:, None], 0.0),
        axis=0,
    )
    gate_slots = to_experts(gate_rows)

    if spread > 1:
        start = rep_at * own
        weight_in = lax.dynamic_slice_in_dim(expert_in, start, own, 0)
        weight_out = lax.dynamic_slice_in_dim(expert_out, start, own, 0)
    else:
        weight_in, weight_out = expert_in, expert_out
    expert_act, expert_slope = gelu_pair(
        jnp.einsum("erd,edf->erf", arrived, weight_in, preferred_element_type=f32)
    )
    expert_act, expert_slope = expert_act.astype(bf16), expert_slope.astype(bf16)
    produced = jnp.einsum(
        "erf,efd->erd", expert_act, weight_out, preferred_element_type=f32
    ).astype(bf16)
    grad_float = grad_slots.astype(f32)
    grad_arrived = (gate_slots[:, :, None] * grad_float).astype(bf16)
    grad_expert_out = jnp.einsum(
        "erf,erd->efd", expert_act, grad_arrived, preferred_element_type=f32
    ).astype(bf16)
    gate_grads = to_tokens(jnp.sum(grad_float * produced.astype(f32), axis=-1))
    grad_act = jnp.einsum("erd,efd->erf", grad_arrived, weight_out, preferred_element_type=f32)
    grad_inner = (grad_act * expert_slope.astype(f32)).astype(bf16)
    grad_sent = jnp.einsum(
        "erf,edf->erd", grad_inner, weight_in, preferred_element_type=f32
    ).astype(bf16)
    grad_returned = to_tokens(grad_sent)
    grad_expert_in = jnp.einsum(
        "erd,erf->edf", arrived, grad_inner, preferred_element_type=f32
    ).astype(bf16)
    returned = to_tokens(produced)

    def complete(finished):
        if spread == 1:
            return lax.psum(finished, "rep").astype(f32)
        if n_rep != 4:
            return lax.all_gather(finished, "rep", axis=0, tiled=True).astype(f32)
        half = finished.shape[1] // 2
        over_x, over_y = [(i, i ^ 1) for i in range(4)], [(i, i ^ 2) for i in range(4)]
        top, bottom = finished[:, :half], finished[:, half:]
        top_x, bottom_y = swap(top, over_x), swap(bottom, over_y)
        bottom_x, top_y = swap(bottom, over_x), swap(top, over_y)
        top_d, bottom_d = swap(top_x, over_y), swap(bottom_y, over_x)
        blocks = jnp.stack(
            [
                jnp.concatenate(pair, axis=1)
                for pair in ((top, bottom), (top_x, bottom_x), (top_y, bottom_y), (top_d, bottom_d))
            ]
        )
        ordered = [
            lax.dynamic_index_in_dim(blocks, e ^ rep_at, 0, keepdims=False) for e in range(4)
        ]
        return jnp.concatenate(ordered, axis=0).astype(f32)

    full_grad_out = complete(grad_expert_out)
    full_grad_in = complete(grad_expert_in)

    first_rows = dense_product(pick_first, returned)
    second_rows = dense_product(pick_second, returned)
    block_out = second + (gate_probs[:, :1] * first_rows + gate_probs[:, 1:] * second_rows)
    top_grad = out_grad.astype(f32)
    grad_gate = jnp.stack(
        [
            jnp.sum(jnp.where(hit_first, gate_grads[None, :], 0.0), axis=1),
            jnp.sum(jnp.where(hit_second, gate_grads[None, :], 0.0), axis=1),
        ],
        axis=1,
    )
    grad_chosen = gate_probs * (grad_gate - jnp.sum(gate_probs * grad_gate, axis=-1, keepdims=True))
    grad_logits = jnp.sum(jnp.where(route_picks, grad_chosen[:, :, None], 0.0), axis=1)
    router_float = full_router.astype(f32)
    grad_normed_three = dense_product(pick_both, grad_returned) + jnp.dot(
        grad_logits, router_float.T, precision=lax.Precision.HIGHEST, preferred_element_type=f32
    )
    grad_router = jnp.dot(
        normed_three.astype(f32).T,
        grad_logits,
        precision=lax.Precision.HIGHEST,
        preferred_element_type=f32,
    )
    grad_second, grad_gain_three, grad_shift_three = norm_back(
        second, gain_third, shift_third, grad_normed_three
    )
    grad_second = top_grad + grad_second

    def shares(partial):
        return lax.psum_scatter(partial.astype(bf16), "grp", scatter_dimension=0, tiled=True)

    grad_branch = grad_second.astype(bf16)
    share_fc2 = shares(rows_product(hidden, grad_branch))
    grad_before = (column_product(grad_branch, full_fc2) * hidden_slope.astype(f32)).astype(bf16)
    share_fc1 = shares(rows_product(normed_two, grad_before))
    grad_after, grad_gain_two, grad_shift_two = norm_back(
        after_attn, gain_second, shift_second, column_product(grad_before, full_fc1)
    )
    grad_after = grad_second + grad_after
    grad_attend = grad_after.astype(bf16)
    share_proj = shares(rows_product(attn_mixed, grad_attend))
    grad_mixed = column_product(grad_attend, full_proj).astype(bf16)
    grad_packed = attend_back(packed, log_total, grad_mixed, scaling)
    share_qkv = shares(rows_product(normed_one, grad_packed))
    grad_stream, grad_gain_one, grad_shift_one = norm_back(
        stream, gain_first, shift_first, column_product(grad_packed, full_qkv)
    )
    grad_in = grad_after + grad_stream
    vectors = jnp.stack(
        [
            grad_gain_one,
            grad_shift_one,
            grad_gain_two,
            grad_shift_two,
            grad_gain_three,
            grad_shift_three,
        ],
        axis=1,
    )
    share_small = shares(jnp.concatenate([grad_router, vectors], axis=1))
    totals = [
        lax.psum(share, "rep").astype(f32)
        for share in (share_qkv, share_proj, share_fc1, share_fc2, share_small)
    ]
    total_small = totals[4]
    return (
        block_out,
        grad_in,
        total_small[:, EXPERTS],
        total_small[:, EXPERTS + 1],
        totals[0],
        totals[1],
        total_small[:, EXPERTS + 2],
        total_small[:, EXPERTS + 3],
        totals[2],
        totals[3],
        total_small[:, EXPERTS + 4],
        total_small[:, EXPERTS + 5],
        total_small[:, :EXPERTS],
        full_grad_in,
        full_grad_out,
    )


def solution(mesh):
    return jax.shard_map(
        functools.partial(local, mesh.shape["rep"], mesh.shape["grp"]),
        mesh=mesh,
        in_specs=(
            P(("rep", "grp"), None),
            P(("rep", "grp"), None),
            P(("rep", "grp"), None),
            P("grp"),
            P("grp"),
            P("grp", None),
            P("grp", None),
            P("grp"),
            P("grp"),
            P("grp", None),
            P("grp", None),
            P("grp"),
            P("grp"),
            P("grp", None),
            P("grp", None, None),
            P("grp", None, None),
        ),
        out_specs=(
            P(("rep", "grp"), None),
            P(("rep", "grp"), None),
            P("grp"),
            P("grp"),
            P("grp", None),
            P("grp", None),
            P("grp"),
            P("grp"),
            P("grp", None),
            P("grp", None),
            P("grp"),
            P("grp"),
            P("grp", None),
            P("grp", None, None),
            P("grp", None, None),
        ),
        check_vma=False,
    )
```

```python
import functools

import jax
import jax.numpy as jnp
from jax import lax
from jax.experimental import pallas as pl
from jax.experimental.pallas import tpu as pltpu
from jax.sharding import PartitionSpec as P


HEADS = 12
HEAD_DIM = 64
EXPERTS = 32
SEQ_LEN = 197
SLOTS = 80


def layer_norm(operand, norm_gain, norm_shift):
    row_mean = jnp.mean(operand, axis=-1, keepdims=True)
    center = operand - row_mean
    spread = jnp.mean(center * center, axis=-1, keepdims=True)
    return center * lax.rsqrt(spread + 1e-06) * norm_gain + norm_shift


def gelu_pair(x):
    below = 0.5 * lax.erf(x * 0.7071067811865476) + 0.5
    return x * below, below + x * (jnp.exp(-0.5 * x * x) * 0.3989422804014327)


def norm_back(operand, norm_gain, norm_shift, upstream):
    _, pullback = jax.vjp(layer_norm, operand, norm_gain, norm_shift)
    return pullback(upstream)


def dense_product(left_side, right_side):
    return jnp.dot(left_side, right_side, preferred_element_type=jnp.float32)


def rows_product(left_side, right_side):
    return lax.dot_general(
        left_side, right_side, (((0,), (0,)), ((), ())), preferred_element_type=jnp.float32
    )


def column_product(left_side, right_side):
    return lax.dot_general(
        left_side, right_side, (((1,), (1,)), ((), ())), preferred_element_type=jnp.float32
    )


def attend(packed, scaling):
    seq_count = packed.shape[0] // SEQ_LEN
    split_heads = packed.reshape(seq_count, SEQ_LEN, 3, HEADS, HEAD_DIM)
    scores = (
        jnp.einsum(
            "bqhd,bkhd->bhqk",
            split_heads[:, :, 0],
            split_heads[:, :, 1],
            preferred_element_type=jnp.float32,
        )
        * scaling
    )
    row_top = jnp.max(scores, axis=-1, keepdims=True)
    exp_scores = jnp.exp(scores - row_top)
    row_total = jnp.sum(exp_scores, axis=-1, keepdims=True)
    softmaxed = (exp_scores / row_total).astype(jnp.bfloat16)
    attn_mixed = jnp.einsum(
        "bhqk,bkhd->bqhd", softmaxed, split_heads[:, :, 2], preferred_element_type=jnp.float32
    )
    return (
        attn_mixed.reshape(packed.shape[0], HEADS * HEAD_DIM).astype(jnp.bfloat16),
        row_top + jnp.log(row_total),
    )


def attend_back(packed, log_total, grad_mixed, scaling):
    seq_count = packed.shape[0] // SEQ_LEN
    split_heads = packed.reshape(seq_count, SEQ_LEN, 3, HEADS, HEAD_DIM)
    queries = split_heads[:, :, 0]
    key_rows = split_heads[:, :, 1]
    value_rows = split_heads[:, :, 2]
    scores = (
        jnp.einsum("bqhd,bkhd->bhqk", queries, key_rows, preferred_element_type=jnp.float32)
        * scaling
    )
    softmaxed = jnp.exp(scores - log_total)
    grad_heads = grad_mixed.reshape(seq_count, SEQ_LEN, HEADS, HEAD_DIM)
    grad_probs = jnp.einsum(
        "bqhd,bkhd->bhqk", grad_heads, value_rows, preferred_element_type=jnp.float32
    )
    grad_values = jnp.einsum(
        "bhqk,bqhd->bkhd",
        softmaxed.astype(jnp.bfloat16),
        grad_heads,
        preferred_element_type=jnp.float32,
    )
    row_inner = jnp.sum(grad_probs * softmaxed, axis=-1, keepdims=True)
    grad_scores = (softmaxed * (grad_probs - row_inner)).astype(jnp.bfloat16)
    grad_queries = (
        jnp.einsum("bhqk,bkhd->bqhd", grad_scores, key_rows, preferred_element_type=jnp.float32)
        * scaling
    )
    grad_keys = (
        jnp.einsum("bhqk,bqhd->bkhd", grad_scores, queries, preferred_element_type=jnp.float32)
        * scaling
    )
    stacked = jnp.stack([grad_queries, grad_keys, grad_values], axis=2)
    return stacked.reshape(packed.shape[0], 3 * HEADS * HEAD_DIM).astype(jnp.bfloat16)


MESH = pl.DeviceIdType.MESH


def gather_kernel(count, *refs):
    shards, outs = refs[:count], refs[count : 2 * count]
    own_sem, z_send, z_recv, a_send, a_recv, b_send, b_recv, d_send, d_recv, c_send, c_recv, s_send, s_recv = refs[2 * count :]
    rep, grp = lax.axis_index("rep"), lax.axis_index("grp")
    y, x = rep // 2, rep % 2
    z, core = grp // 2, grp % 2
    a_y, a_x = (1 - core) * y + core * (1 - y), core * x + (1 - core) * (1 - x)
    b_y, b_x = core * y + (1 - core) * (1 - y), (1 - core) * x + core * (1 - x)
    at_a, at_b, at_d = 2 * a_y + a_x, 2 * b_y + b_x, 2 * (1 - y) + (1 - x)
    mate = 2 * z + 1 - core
    others = [(z + step) % 4 for step in (1, 2, 3)]

    barrier = pltpu.get_barrier_semaphore()
    for target in [(rep, 2 * there + core) for there in others] + [(at_a, grp), (at_b, grp), (rep, mate)]:
        pl.semaphore_signal(barrier, inc=1, device_id=target, device_id_type=MESH)
    pl.semaphore_wait(barrier, 6)

    def send(source, sink, send_sem, recv_sem, target):
        copy = pltpu.make_async_remote_copy(
            src_ref=source, dst_ref=sink, send_sem=send_sem, recv_sem=recv_sem, device_id=target, device_id_type=MESH
        )
        copy.start()
        return copy

    sent, local = [], []
    from_z, from_a, from_b, from_d, from_mate, whole = [], [], [], [], [], []
    for k in range(count):
        for i, there in enumerate(others):
            copy = send(shards[k].at[rep], outs[k].at[grp, rep], z_send.at[k, i], z_recv.at[k, i], (rep, 2 * there + core))
            from_z.append(copy)
            sent.append(copy)
    for k in range(count):
        copy = send(shards[k], outs[k].at[grp], s_send.at[k], s_recv.at[k], (rep, mate))
        sent.append(copy)
        whole.append(copy)
        mine = pltpu.make_async_copy(shards[k], outs[k].at[grp], own_sem.at[k])
        mine.start()
        local.append(mine)
    sources = [2 * ((z + 4 - step) % 4) + core for step in (1, 2, 3)]
    for k in range(count):
        for i, origin in enumerate(sources):
            from_z[3 * k + i].wait_recv()
            piece = outs[k].at[origin, rep]
            copy = send(piece, piece, a_send.at[k, i], a_recv.at[k, i], (at_a, grp))
            from_a.append(copy)
            sent.append(copy)
            copy = send(piece, piece, b_send.at[k, i], b_recv.at[k, i], (at_b, grp))
            from_b.append(copy)
            sent.append(copy)
            copy = send(piece, piece, c_send.at[k, 0, i], c_recv.at[k, 0, i], (rep, mate))
            from_mate.append(copy)
            sent.append(copy)
    for k in range(count):
        for i, origin in enumerate(sources):
            from_a[3 * k + i].wait_recv()
            piece = outs[k].at[origin, at_a]
            copy = send(piece, piece, d_send.at[k, i], d_recv.at[k, i], (at_b, grp))
            from_d.append(copy)
            sent.append(copy)
            copy = send(piece, piece, c_send.at[k, 1, i], c_recv.at[k, 1, i], (rep, mate))
            from_mate.append(copy)
            sent.append(copy)
            from_b[3 * k + i].wait_recv()
            piece = outs[k].at[origin, at_b]
            copy = send(piece, piece, c_send.at[k, 2, i], c_recv.at[k, 2, i], (rep, mate))
            from_mate.append(copy)
            sent.append(copy)
    for k in range(count):
        for i, origin in enumerate(sources):
            from_d[3 * k + i].wait_recv()
            piece = outs[k].at[origin, at_d]
            copy = send(piece, piece, c_send.at[k, 3, i], c_recv.at[k, 3, i], (rep, mate))
            from_mate.append(copy)
            sent.append(copy)
    for copy in whole + from_mate:
        copy.wait_recv()
    for copy in sent:
        copy.wait_send()
    for copy in local:
        copy.wait()


def gather_dense(shards, collective_id):
    count = len(shards)
    views = [shard.reshape(4, shard.shape[0] // 4, shard.shape[1]) for shard in shards]
    dma = pltpu.SemaphoreType.DMA
    moved = sum(view.size * 2 for view in views)
    outs = pl.pallas_call(
        functools.partial(gather_kernel, count),
        out_shape=[jax.ShapeDtypeStruct((8,) + view.shape, view.dtype) for view in views],
        in_specs=[pl.BlockSpec(memory_space=pltpu.VMEM)] * count,
        out_specs=[pl.BlockSpec(memory_space=pl.ANY)] * count,
        scratch_shapes=[dma((count,))] + [dma((count, 3))] * 8 + [dma((count, 4, 3))] * 2 + [dma((count,))] * 2,
        compiler_params=pltpu.CompilerParams(collective_id=collective_id, has_side_effects=True),
        cost_estimate=pl.CostEstimate(flops=0, bytes_accessed=16 * moved, transcendentals=0),
        name="gather_dense",
    )(*views)
    return [out.reshape(8 * shard.shape[0], shard.shape[1]) for out, shard in zip(outs, shards)]


BF16, F32 = jnp.bfloat16, jnp.float32
ROW_TILE = 1280
FEATURE_TILE = 512


def transposed_product(left_side, right_side):
    return lax.dot_general(
        left_side, right_side, (((1,), (1,)), ((), ())), preferred_element_type=F32
    )


def expert_forward_kernel(at, rows, grads_t, weight, *refs):
    act, slope, share, total = refs[-4:]
    for tile in range(rows.shape[0] // ROW_TILE):
        span = pl.ds(tile * ROW_TILE, ROW_TILE)
        value, turn = gelu_pair(dense_product(rows[span, :], weight[...]))
        value = value.astype(BF16)
        act[span, :] = value
        slope[span, :] = turn.astype(BF16)
        part = dense_product(grads_t[:, span], value)
        if tile == 0:
            total[...] = part
        else:
            total[...] += part
    share[...] = total[...].T.astype(BF16)


def expert_forward(at, rows, grads_t, weight, first, count, held):
    slots, width = rows.shape
    units = weight.shape[2]
    base = first // FEATURE_TILE
    whole = pl.BlockSpec(rows.shape, lambda i, at: (0, 0), pipeline_mode=pl.Buffered(1))
    whole_t = pl.BlockSpec(grads_t.shape, lambda i, at: (0, 0), pipeline_mode=pl.Buffered(1))
    side = pl.BlockSpec((slots, FEATURE_TILE), lambda i, at: (0, base + i))
    return pl.pallas_call(
        expert_forward_kernel,
        out_shape=[
            jax.ShapeDtypeStruct((slots, units), BF16),
            jax.ShapeDtypeStruct((slots, units), BF16),
            jax.ShapeDtypeStruct((count, width), BF16),
        ],
        grid_spec=pltpu.PrefetchScalarGridSpec(
            num_scalar_prefetch=1,
            grid=(count // FEATURE_TILE,),
            in_specs=[
                whole,
                whole_t,
                pl.BlockSpec((None, width, FEATURE_TILE), lambda i, at: (at[0], 0, base + i)),
            ]
            + [pl.BlockSpec(memory_space=pl.ANY)] * len(held),
            out_specs=[side, side, pl.BlockSpec((FEATURE_TILE, width), lambda i, at: (i, 0))],
            scratch_shapes=[pltpu.VMEM((width, FEATURE_TILE), F32)],
        ),
        input_output_aliases={4 + k: k for k in range(len(held))},
        compiler_params=pltpu.CompilerParams(vmem_limit_bytes=60 << 20),
        cost_estimate=pl.CostEstimate(
            flops=4 * slots * width * count,
            bytes_accessed=4 * slots * width + 4 * slots * count + 4 * width * count,
            transcendentals=2 * slots * count,
        ),
        name="expert_forward",
    )(at, rows, grads_t, weight, *held)


def expert_backward_kernel(
    at, grads, weight_in, weight_out, act, slope, inner, made, sent, made_sum, sent_sum
):
    step = pl.program_id(0)

    @pl.when(step == 0)
    def _():
        made_sum[...] = jnp.zeros_like(made_sum)
        sent_sum[...] = jnp.zeros_like(sent_sum)

    for tile in range(grads.shape[0] // ROW_TILE):
        span = pl.ds(tile * ROW_TILE, ROW_TILE)
        value = transposed_product(grads[span, :], weight_out[...]) * slope[span, :].astype(F32)
        value = value.astype(BF16)
        inner[span, :] = value
        sent_sum[span, :] += transposed_product(value, weight_in[...])
        made_sum[span, :] += dense_product(act[span, :], weight_out[...])

    @pl.when(step == pl.num_programs(0) - 1)
    def _():
        made[...] = made_sum[...].astype(BF16)
        sent[...] = sent_sum[...].astype(BF16)


def expert_backward(at, grads, weight_in, weight_out, act, slope):
    slots, width = grads.shape
    units = weight_in.shape[2]
    whole = pl.BlockSpec(grads.shape, lambda i, at: (0, 0), pipeline_mode=pl.Buffered(1))
    side = pl.BlockSpec((slots, FEATURE_TILE), lambda i, at: (0, i))
    return pl.pallas_call(
        expert_backward_kernel,
        out_shape=[
            jax.ShapeDtypeStruct((slots, units), BF16),
            jax.ShapeDtypeStruct((slots, width), BF16),
            jax.ShapeDtypeStruct((slots, width), BF16),
        ],
        grid_spec=pltpu.PrefetchScalarGridSpec(
            num_scalar_prefetch=1,
            grid=(units // FEATURE_TILE,),
            in_specs=[
                whole,
                pl.BlockSpec((None, width, FEATURE_TILE), lambda i, at: (at[0], 0, i)),
                pl.BlockSpec((None, FEATURE_TILE, width), lambda i, at: (at[0], i, 0)),
                side,
                side,
            ],
            out_specs=[side, whole, whole],
            scratch_shapes=[pltpu.VMEM((slots, width), F32)] * 2,
        ),
        compiler_params=pltpu.CompilerParams(vmem_limit_bytes=63 << 20),
        cost_estimate=pl.CostEstimate(
            flops=6 * slots * width * units,
            bytes_accessed=6 * slots * width + 6 * slots * units + 4 * width * units,
            transcendentals=0,
        ),
        name="expert_backward",
    )(at, grads, weight_in, weight_out, act, slope)


def expert_gradient_kernel(rows_t, inner, top, bottom):
    total = dense_product(rows_t[...], inner[...])
    half = total.shape[0] // 2
    top[...] = total[:half, :].astype(BF16)
    bottom[...] = total[half:, :].astype(BF16)


def expert_gradient(rows_t, inner):
    width, slots = rows_t.shape
    units = inner.shape[1]
    half = pl.BlockSpec((width // 2, FEATURE_TILE), lambda i: (0, i))
    return pl.pallas_call(
        expert_gradient_kernel,
        out_shape=[jax.ShapeDtypeStruct((width // 2, units), BF16)] * 2,
        grid=(units // FEATURE_TILE,),
        in_specs=[
            pl.BlockSpec(rows_t.shape, lambda i: (0, 0), pipeline_mode=pl.Buffered(1)),
            pl.BlockSpec((slots, FEATURE_TILE), lambda i: (0, i)),
        ],
        out_specs=[half, half],
        compiler_params=pltpu.CompilerParams(vmem_limit_bytes=60 << 20),
        cost_estimate=pl.CostEstimate(
            flops=2 * slots * width * units,
            bytes_accessed=2 * slots * width + 2 * slots * units + 2 * width * units,
            transcendentals=0,
        ),
        name="expert_gradient",
    )(rows_t, inner)


def scatter_kernel(grad, out, mated, halves, planar, quarters, lined, done, sems):
    m_send, m_recv, p_send, p_recv, l_send, l_recv, d_send, d_recv = sems
    rep, grp = lax.axis_index("rep"), lax.axis_index("grp")
    y, x = rep // 2, rep % 2
    z, core = grp // 2, grp % 2
    plane = [2 * y + 1 - x, 2 * (1 - y) + x, 2 * (1 - y) + 1 - x]
    line = [(z + step) % 4 for step in (1, 2, 3)]
    mate = (rep, 2 * z + 1 - core)

    barrier = pltpu.get_barrier_semaphore()
    for target in [mate] + [(there, grp) for there in plane] + [(rep, 2 * k + core) for k in line]:
        pl.semaphore_signal(barrier, inc=1, device_id=target, device_id_type=MESH)
    pl.semaphore_wait(barrier, 7)

    def send(source, sink, send_sem, recv_sem, target):
        copy = pltpu.make_async_remote_copy(
            src_ref=source,
            dst_ref=sink,
            send_sem=send_sem,
            recv_sem=recv_sem,
            device_id=target,
            device_id_type=MESH,
        )
        copy.start()
        return copy

    to_mate = [
        send(grad.at[k, 1 - core], mated.at[k], m_send.at[k], m_recv.at[k], mate) for k in range(4)
    ]
    to_plane = []
    for k in range(4):
        to_mate[k].wait_recv()
        for q in range(4):
            total = grad[k, core, q].astype(F32) + mated[k, q].astype(F32)
            halves[k, q] = total.astype(BF16)
        to_plane.append(
            [
                send(
                    halves.at[k, there],
                    planar.at[i, k],
                    p_send.at[i, k],
                    p_recv.at[i, k],
                    (there, grp),
                )
                for i, there in enumerate(plane)
            ]
        )
    to_line = []
    for k in range(4):
        for copy in to_plane[k]:
            copy.wait_recv()
        total = halves[k, rep].astype(F32)
        for i in range(3):
            total += planar[i, k].astype(F32)
        quarters[k] = total.astype(BF16)
    for i, there in enumerate(line):
        to_line.append(
            send(
                quarters.at[there],
                lined.at[i],
                l_send.at[i],
                l_recv.at[i],
                (rep, 2 * there + core),
            )
        )
    total = quarters[z].astype(F32)
    for i in range(3):
        to_line[i].wait_recv()
        total += lined[i].astype(F32)
    done[rep] = total.astype(BF16)
    to_all = [
        send(done.at[rep], done.at[rep], d_send.at[i], d_recv.at[i], (there, grp))
        for i, there in enumerate(plane)
    ]
    for copy in to_all:
        copy.wait_recv()
    for q in range(4):
        out[q] = done[q].astype(F32)
    for copy in to_mate + [copy for row in to_plane for copy in row] + to_line + to_all:
        copy.wait_send()


def scatter_dense(grad, collective_id):
    rows, columns = grad.shape[0] // 32, grad.shape[1]
    dma = pltpu.SemaphoreType.DMA
    block = (rows, columns)

    def kernel(grad, out, mated, halves, planar, quarters, lined, done, *sems):
        scatter_kernel(grad, out, mated, halves, planar, quarters, lined, done, sems)

    out = pl.pallas_call(
        kernel,
        out_shape=jax.ShapeDtypeStruct((4,) + block, F32),
        in_specs=[pl.BlockSpec(memory_space=pltpu.VMEM)],
        out_specs=pl.BlockSpec(memory_space=pltpu.VMEM),
        scratch_shapes=[
            pltpu.VMEM((4, 4) + block, BF16),
            pltpu.VMEM((4, 4) + block, BF16),
            pltpu.VMEM((3, 4) + block, BF16),
            pltpu.VMEM((4,) + block, BF16),
            pltpu.VMEM((3,) + block, BF16),
            pltpu.VMEM((4,) + block, BF16),
        ]
        + [dma((4,))] * 2
        + [dma((3, 4))] * 2
        + [dma((3,))] * 4,
        compiler_params=pltpu.CompilerParams(
            collective_id=collective_id, has_side_effects=True, vmem_limit_bytes=60 << 20
        ),
        cost_estimate=pl.CostEstimate(flops=0, bytes_accessed=64 * rows * columns, transcendentals=0),
        name="scatter_dense",
    )(grad.reshape((4, 2, 4) + block))
    return out.reshape(4 * rows, columns)


def place_kernel(at, piece, *refs):
    refs[-1][...] = piece[...].astype(F32)


def place(held, piece, expert, count, shape, row, column):
    rows, columns = piece.shape
    tile = rows // 3 if columns > 1024 else rows // 2
    in_specs = [pl.BlockSpec((tile, columns), lambda i, at: (i, 0))]
    operands = [expert.reshape(1), piece]
    if held is not None:
        in_specs.append(pl.BlockSpec(memory_space=pl.ANY))
        operands.append(held)
    return pl.pallas_call(
        place_kernel,
        out_shape=jax.ShapeDtypeStruct((count,) + shape, F32),
        grid_spec=pltpu.PrefetchScalarGridSpec(
            num_scalar_prefetch=1,
            grid=(rows // tile,),
            in_specs=in_specs,
            out_specs=pl.BlockSpec(
                (None, tile, columns), lambda i, at: (at[0], row // tile + i, column // columns)
            ),
        ),
        input_output_aliases={2: 0} if held is not None else {},
        cost_estimate=pl.CostEstimate(
            flops=0, bytes_accessed=6 * rows * columns, transcendentals=0
        ),
        name="place",
    )(*operands)


def complete(rep_at, top, bottom, shape):
    half = shape[0] // 2
    over_x, over_y = [(i, i ^ 1) for i in range(4)], [(i, i ^ 2) for i in range(4)]
    top_x, top_y = swap(top, over_x), swap(top, over_y)
    bottom_y, bottom_x = (swap(bottom, over_y), swap(bottom, over_x))
    top_d, bottom_d = (swap(top_x, over_y), swap(bottom_y, over_x))
    held = None
    for away, row, piece in (
        (0, 0, top),
        (0, half, bottom),
        (1, 0, top_x),
        (2, 0, top_y),
        (2, half, bottom_y),
        (1, half, bottom_x),
        (3, 0, top_d),
        (3, half, bottom_d),
    ):
        held = place(held, piece, rep_at ^ away, 4, shape, row, 0)
    return held


def swap(operand, axis_pairs):
    return lax.ppermute(operand, "rep", axis_pairs)


def local(
    n_rep,
    n_grp,
    block_in,
    out_grad,
    routes,
    ln1_gain,
    ln1_bias,
    w_qkv,
    w_proj,
    ln2_gain,
    ln2_bias,
    w_fc1,
    w_fc2,
    ln3_gain,
    ln3_bias,
    w_router,
    expert_in,
    expert_out,
):
    bf16, f32 = jnp.bfloat16, jnp.float32
    scaling = HEAD_DIM ** (-0.5)
    tok_rows, width = block_in.shape
    held = expert_in.shape[0]
    spread = n_rep if held % n_rep == 0 else 1
    own = held // spread
    axes = ("rep", "grp") if spread > 1 else ("grp",)
    peers = spread * n_grp
    rep_at = lax.axis_index("rep")

    def gather(shard):
        return lax.all_gather(shard, "grp", axis=0, tiled=True)

    vectors = jnp.stack([ln1_gain, ln1_bias, ln2_gain, ln2_bias, ln3_gain, ln3_bias], axis=1)
    narrow = jnp.concatenate([w_router, vectors], axis=1)
    if n_rep == 4 and n_grp == 8:
        lanes = 128 - narrow.shape[1]
        joint = jnp.concatenate([w_qkv, w_proj, jnp.pad(narrow, ((0, 0), (0, lanes)))], axis=1)
        joint, full_fc1, full_fc2 = gather_dense([joint, w_fc1, w_fc2], 0)
        full_qkv = joint[:, : 3 * width]
        full_proj = joint[:, 3 * width : 4 * width]
        narrow = joint[:, 4 * width :]
    else:
        full_qkv, full_proj, full_fc1, full_fc2, narrow = map(
            gather, (w_qkv, w_proj, w_fc1, w_fc2, narrow)
        )
    full_router, small = narrow[:, :EXPERTS], narrow[:, EXPERTS : EXPERTS + 6]
    small = small.astype(f32).T
    gain_first, shift_first, gain_second, shift_second, gain_third, shift_third = small

    expert_ids = lax.iota(jnp.int32, EXPERTS)
    route_picks = routes[:, :, None] == expert_ids[None, None, :]
    hits = jnp.any(route_picks, axis=1)
    earlier = (
        lax.broadcasted_iota(jnp.int32, (tok_rows, tok_rows), 1)
        < lax.broadcasted_iota(jnp.int32, (tok_rows, tok_rows), 0)
    ).astype(bf16)
    ranks = dense_product(earlier, hits.astype(bf16)).astype(jnp.int32)
    rank = jnp.sum(jnp.where(route_picks, ranks[:, None, :], 0), axis=-1)
    group_of, within = routes // held, routes % held
    place = ((within // own) * n_grp + group_of) * own + within % own
    slot = place * SLOTS + rank
    slot_ids = lax.iota(jnp.int32, EXPERTS * SLOTS)
    pick_first = (slot[:, 0][:, None] == slot_ids[None, :]).astype(bf16)
    pick_second = (slot[:, 1][:, None] == slot_ids[None, :]).astype(bf16)
    pick_both = pick_first + pick_second

    def exchange(rows):
        return lax.all_to_all(rows, axes, split_axis=0, concat_axis=0, tiled=True)

    def to_experts(rows):
        rows = exchange(rows.reshape((peers, own, SLOTS) + rows.shape[1:]))
        return jnp.moveaxis(rows, 1, 0).reshape((own, peers * SLOTS) + rows.shape[3:])

    def to_tokens(rows):
        rows = jnp.moveaxis(rows.reshape((own, peers, SLOTS) + rows.shape[2:]), 1, 0)
        return exchange(rows).reshape((EXPERTS * SLOTS,) + rows.shape[3:])

    grad_slots = to_experts(rows_product(pick_both, out_grad).astype(bf16))

    stream = block_in.astype(f32)
    normed_one = layer_norm(stream, gain_first, shift_first).astype(bf16)
    packed = dense_product(normed_one, full_qkv).astype(bf16)
    attn_mixed, log_total = attend(packed, scaling)
    after_attn = stream + dense_product(attn_mixed, full_proj)
    normed_two = layer_norm(after_attn, gain_second, shift_second).astype(bf16)
    hidden, hidden_slope = gelu_pair(dense_product(normed_two, full_fc1))
    hidden, hidden_slope = hidden.astype(bf16), hidden_slope.astype(bf16)
    second = after_attn + dense_product(hidden, full_fc2)
    normed_three = layer_norm(second, gain_third, shift_third).astype(bf16)
    arrived = to_experts(rows_product(pick_both, normed_three).astype(bf16))

    logits = dense_product(normed_three, full_router)
    chosen = jnp.sum(jnp.where(route_picks, logits[:, None, :], 0.0), axis=-1)
    chosen_exp = jnp.exp(chosen - jnp.max(chosen, axis=-1, keepdims=True))
    gate_probs = chosen_exp / jnp.sum(chosen_exp, axis=-1, keepdims=True)
    hit_first = slot[:, 0][:, None] == slot_ids[None, :]
    hit_second = slot[:, 1][:, None] == slot_ids[None, :]
    gate_rows = jnp.sum(
        jnp.where(hit_first, gate_probs[:, 0][:, None], 0.0)
        + jnp.where(hit_second, gate_probs[:, 1][:, None], 0.0),
        axis=0,
    )
    gate_slots = to_experts(gate_rows)

    grad_float = grad_slots.astype(f32)
    grad_arrived = (gate_slots[:, :, None] * grad_float).astype(bf16)
    half = expert_in.shape[2] // 2
    made, sent_back, out_parts, in_parts = [], [], [], []
    for j in range(own):
        at = (rep_at * own + j if spread > 1 else jnp.int32(j)).reshape(1).astype(jnp.int32)
        rows, grads = arrived[j], grad_arrived[j]
        raw_t = lax.optimization_barrier(grad_slots[j].T)
        grads_t = (gate_slots[j][None, :] * raw_t.astype(f32)).astype(bf16)
        act, slope, out_top = expert_forward(at, rows, grads_t, expert_in, 0, half, ())
        act, slope, out_bottom = expert_forward(
            at, rows, grads_t, expert_in, half, half, (act, slope)
        )
        inner, result, back = expert_backward(at, grads, expert_in, expert_out, act, slope)
        in_top, in_bottom = expert_gradient(rows.T, inner)
        out_parts.append((out_top, out_bottom))
        in_parts.append((in_top, in_bottom))
        made.append(result)
        sent_back.append(back)
    produced, grad_sent = jnp.stack(made), jnp.stack(sent_back)
    gate_grads = to_tokens(jnp.sum(grad_float * produced.astype(f32), axis=-1))
    grad_returned = to_tokens(grad_sent)
    returned = to_tokens(produced)

    def finish(parts, shape):
        if spread == 4 and own == 1:
            return complete(rep_at, parts[0][0], parts[0][1], shape)
        finished = jnp.stack([jnp.concatenate(pair) for pair in parts])
        if spread > 1:
            return lax.all_gather(finished, "rep", axis=0, tiled=True).astype(f32)
        return lax.psum(finished, "rep").astype(f32)

    full_grad_out = finish(out_parts, expert_out.shape[1:])
    full_grad_in = finish(in_parts, expert_in.shape[1:])

    first_rows = dense_product(pick_first, returned)
    second_rows = dense_product(pick_second, returned)
    block_out = second + (gate_probs[:, :1] * first_rows + gate_probs[:, 1:] * second_rows)
    top_grad = out_grad.astype(f32)
    grad_gate = jnp.stack(
        [
            jnp.sum(jnp.where(hit_first, gate_grads[None, :], 0.0), axis=1),
            jnp.sum(jnp.where(hit_second, gate_grads[None, :], 0.0), axis=1),
        ],
        axis=1,
    )
    grad_chosen = gate_probs * (grad_gate - jnp.sum(gate_probs * grad_gate, axis=-1, keepdims=True))
    grad_logits = jnp.sum(jnp.where(route_picks, grad_chosen[:, :, None], 0.0), axis=1)
    router_float = full_router.astype(f32)
    grad_normed_three = dense_product(pick_both, grad_returned) + jnp.dot(
        grad_logits, router_float.T, precision=lax.Precision.HIGHEST, preferred_element_type=f32
    )
    grad_router = jnp.dot(
        normed_three.astype(f32).T,
        grad_logits,
        precision=lax.Precision.HIGHEST,
        preferred_element_type=f32,
    )
    grad_second, grad_gain_three, grad_shift_three = norm_back(
        second, gain_third, shift_third, grad_normed_three
    )
    grad_second = top_grad + grad_second

    def shares(partial):
        return lax.psum_scatter(partial.astype(bf16), "grp", scatter_dimension=0, tiled=True)

    grad_branch = grad_second.astype(bf16)
    grad_fc2 = rows_product(hidden, grad_branch).astype(bf16)
    share_fc2 = shares(grad_fc2)
    grad_before = (column_product(grad_branch, full_fc2) * hidden_slope.astype(f32)).astype(bf16)
    grad_fc1 = rows_product(normed_two, grad_before).astype(bf16)
    share_fc1 = shares(grad_fc1)
    grad_after, grad_gain_two, grad_shift_two = norm_back(
        after_attn, gain_second, shift_second, column_product(grad_before, full_fc1)
    )
    grad_after = grad_second + grad_after
    grad_attend = grad_after.astype(bf16)
    grad_proj = rows_product(attn_mixed, grad_attend).astype(bf16)
    grad_mixed = column_product(grad_attend, full_proj).astype(bf16)
    grad_packed = attend_back(packed, log_total, grad_mixed, scaling)
    grad_qkv = rows_product(normed_one, grad_packed).astype(bf16)
    grad_stream, grad_gain_one, grad_shift_one = norm_back(
        stream, gain_first, shift_first, column_product(grad_packed, full_qkv)
    )
    grad_in = grad_after + grad_stream
    vectors = jnp.stack(
        [
            grad_gain_one,
            grad_shift_one,
            grad_gain_two,
            grad_shift_two,
            grad_gain_three,
            grad_shift_three,
        ],
        axis=1,
    )
    narrow = jnp.concatenate([grad_router, vectors], axis=1).astype(bf16)
    if n_rep == 4 and n_grp == 8:
        lanes = 128 - narrow.shape[1]
        joint = jnp.concatenate(
            [grad_qkv, grad_proj, jnp.pad(narrow, ((0, 0), (0, lanes)))], axis=1
        )
        joint = scatter_dense(joint, 1)
        total_qkv = joint[:, : 3 * width]
        total_proj = joint[:, 3 * width : 4 * width]
        total_small = joint[:, 4 * width :]
    else:
        total_qkv, total_proj, total_small = (
            lax.psum(shares(part), "rep").astype(f32) for part in (grad_qkv, grad_proj, narrow)
        )
    total_fc1, total_fc2 = (lax.psum(share, "rep").astype(f32) for share in (share_fc1, share_fc2))
    return (
        block_out,
        grad_in,
        total_small[:, EXPERTS],
        total_small[:, EXPERTS + 1],
        total_qkv,
        total_proj,
        total_small[:, EXPERTS + 2],
        total_small[:, EXPERTS + 3],
        total_fc1,
        total_fc2,
        total_small[:, EXPERTS + 4],
        total_small[:, EXPERTS + 5],
        total_small[:, :EXPERTS],
        full_grad_in,
        full_grad_out,
    )


def solution(mesh):
    return jax.shard_map(
        functools.partial(local, mesh.shape["rep"], mesh.shape["grp"]),
        mesh=mesh,
        in_specs=(
            P(("rep", "grp"), None),
            P(("rep", "grp"), None),
            P(("rep", "grp"), None),
            P("grp"),
            P("grp"),
            P("grp", None),
            P("grp", None),
            P("grp"),
            P("grp"),
            P("grp", None),
            P("grp", None),
            P("grp"),
            P("grp"),
            P("grp", None),
            P("grp", None, None),
            P("grp", None, None),
        ),
        out_specs=(
            P(("rep", "grp"), None),
            P(("rep", "grp"), None),
            P("grp"),
            P("grp"),
            P("grp", None),
            P("grp", None),
            P("grp"),
            P("grp"),
            P("grp", None),
            P("grp", None),
            P("grp"),
            P("grp"),
            P("grp", None),
            P("grp", None, None),
            P("grp", None, None),
        ),
        check_vma=False,
    )
```

```python
import functools

import jax
import jax.numpy as jnp
from jax import lax
from jax.experimental import pallas as pl
from jax.experimental.pallas import tpu as pltpu
from jax.sharding import PartitionSpec as P


HEADS = 12
HEAD_DIM = 64
EXPERTS = 32
SEQ_LEN = 197
SLOTS = 80
BF16, F32 = jnp.bfloat16, jnp.float32


def layer_norm(operand, norm_gain, norm_shift):
    row_mean = jnp.mean(operand, axis=-1, keepdims=True)
    center = operand - row_mean
    spread = jnp.mean(center * center, axis=-1, keepdims=True)
    return center * lax.rsqrt(spread + 1e-06) * norm_gain + norm_shift


def gelu_pair(x):
    below = 0.5 * lax.erf(x * 0.7071067811865476) + 0.5
    return x * below, below + x * (jnp.exp(-0.5 * x * x) * 0.3989422804014327)


def norm_back(operand, norm_gain, norm_shift, upstream):
    _, pullback = jax.vjp(layer_norm, operand, norm_gain, norm_shift)
    return pullback(upstream)


def dense_product(left_side, right_side):
    return jnp.dot(left_side, right_side, preferred_element_type=jnp.float32)


def rows_product(left_side, right_side):
    return lax.dot_general(
        left_side, right_side, (((0,), (0,)), ((), ())), preferred_element_type=jnp.float32
    )


def column_product(left_side, right_side):
    return lax.dot_general(
        left_side, right_side, (((1,), (1,)), ((), ())), preferred_element_type=jnp.float32
    )


def head_lanes(shape):
    first = lax.broadcasted_iota(jnp.int32, shape, 1) < HEAD_DIM
    return first, jnp.logical_not(first)


def softmax_rows(scores):
    grown = jnp.exp(scores - jnp.max(scores, axis=-1, keepdims=True))
    return grown * (1.0 / jnp.sum(grown, axis=-1, keepdims=True))


def attend_kernel(scaling, queries, key_rows, values, mixed, wide_q, wide_k, wide_v, wide_o):
    wide_q[...] = queries[...].astype(F32) * scaling
    wide_k[...] = key_rows[...].astype(F32)
    wide_v[...] = values[...].astype(F32)
    heads = head_lanes((SEQ_LEN, queries.shape[1]))
    for image in range(queries.shape[0] // SEQ_LEN):
        span = pl.ds(image * SEQ_LEN, SEQ_LEN)
        q, k, v = wide_q[span, :], wide_k[span, :].astype(BF16), wide_v[span, :]
        total = None
        for lanes in heads:
            probs = softmax_rows(
                transposed_product(jnp.where(lanes, q, 0.0).astype(BF16), k)
            ).astype(BF16)
            part = dense_product(probs, jnp.where(lanes, v, 0.0).astype(BF16))
            total = part if total is None else total + part
        wide_o[span, :] = total
    mixed[...] = wide_o[...].astype(BF16)


def attend(packed, scaling):
    rows, columns = packed.shape
    lanes = 2 * HEAD_DIM
    steps = columns // 3 // lanes

    def block(part):
        return pl.BlockSpec((rows, lanes), lambda h: (0, part * steps + h))

    return pl.pallas_call(
        functools.partial(attend_kernel, scaling),
        out_shape=jax.ShapeDtypeStruct((rows, columns // 3), BF16),
        grid=(steps,),
        in_specs=[block(0), block(1), block(2)],
        out_specs=block(0),
        scratch_shapes=[pltpu.VMEM((rows, lanes), F32)] * 4,
        cost_estimate=pl.CostEstimate(
            flops=4 * rows * SEQ_LEN * columns // 3,
            bytes_accessed=8 * rows * columns // 3,
            transcendentals=rows * SEQ_LEN * HEADS,
        ),
        name="attend",
    )(packed, packed, packed)


def attend_back_kernel(scaling, queries, key_rows, values, grads, grad_q, grad_k, grad_v, *wides):
    wide_q, wide_k, wide_v, wide_g, out_q, out_k, out_v = wides
    wide_q[...] = queries[...].astype(F32) * scaling
    wide_k[...] = key_rows[...].astype(F32)
    wide_v[...] = values[...].astype(F32)
    wide_g[...] = grads[...].astype(F32)
    heads = head_lanes((SEQ_LEN, queries.shape[1]))
    for image in range(queries.shape[0] // SEQ_LEN):
        span = pl.ds(image * SEQ_LEN, SEQ_LEN)
        q, k, v, g = wide_q[span, :], wide_k[span, :], wide_v[span, :], wide_g[span, :]
        k_all, v_all = k.astype(BF16), v.astype(BF16)
        sums = [None, None, None]
        for lanes in heads:
            q_one = jnp.where(lanes, q, 0.0).astype(BF16)
            k_one = jnp.where(lanes, k, 0.0).astype(BF16)
            g_one = jnp.where(lanes, g, 0.0).astype(BF16)
            probs = softmax_rows(transposed_product(q_one, k_all))
            grad_probs = transposed_product(g_one, v_all)
            inner = jnp.sum(grad_probs * probs, axis=-1, keepdims=True)
            grad_scores = (probs * (grad_probs - inner)).astype(BF16)
            parts = (
                dense_product(grad_scores, k_one),
                rows_product(grad_scores, q_one),
                rows_product(probs.astype(BF16), g_one),
            )
            sums = [part if held is None else held + part for held, part in zip(sums, parts)]
        out_q[span, :] = sums[0] * scaling
        out_k[span, :] = sums[1]
        out_v[span, :] = sums[2]
    grad_q[...] = out_q[...].astype(BF16)
    grad_k[...] = out_k[...].astype(BF16)
    grad_v[...] = out_v[...].astype(BF16)


def attend_back(packed, grad_mixed, scaling):
    rows, columns = packed.shape
    lanes = 2 * HEAD_DIM
    steps = columns // 3 // lanes

    def block(part):
        return pl.BlockSpec((rows, lanes), lambda h: (0, part * steps + h))

    return pl.pallas_call(
        functools.partial(attend_back_kernel, scaling),
        out_shape=[jax.ShapeDtypeStruct((rows, columns // 3), BF16)] * 3,
        grid=(steps,),
        in_specs=[block(0), block(1), block(2), block(0)],
        out_specs=[block(0)] * 3,
        scratch_shapes=[pltpu.VMEM((rows, lanes), F32)] * 7,
        cost_estimate=pl.CostEstimate(
            flops=10 * rows * SEQ_LEN * columns // 3,
            bytes_accessed=14 * rows * columns // 3,
            transcendentals=rows * SEQ_LEN * HEADS,
        ),
        name="attend_back",
    )(packed, packed, packed, grad_mixed)


MESH = pl.DeviceIdType.MESH


def gather_kernel(count, *refs):
    shards, outs = refs[:count], refs[count : 2 * count]
    own_sem, z_send, z_recv, a_send, a_recv, b_send, b_recv, d_send, d_recv, c_send, c_recv, s_send, s_recv = refs[2 * count :]
    rep, grp = lax.axis_index("rep"), lax.axis_index("grp")
    y, x = rep // 2, rep % 2
    z, core = grp // 2, grp % 2
    a_y, a_x = (1 - core) * y + core * (1 - y), core * x + (1 - core) * (1 - x)
    b_y, b_x = core * y + (1 - core) * (1 - y), (1 - core) * x + core * (1 - x)
    at_a, at_b, at_d = 2 * a_y + a_x, 2 * b_y + b_x, 2 * (1 - y) + (1 - x)
    mate = 2 * z + 1 - core
    others = [(z + step) % 4 for step in (1, 2, 3)]

    barrier = pltpu.get_barrier_semaphore()
    for target in [(rep, 2 * there + core) for there in others] + [(at_a, grp), (at_b, grp), (rep, mate)]:
        pl.semaphore_signal(barrier, inc=1, device_id=target, device_id_type=MESH)
    pl.semaphore_wait(barrier, 6)

    def send(source, sink, send_sem, recv_sem, target):
        copy = pltpu.make_async_remote_copy(
            src_ref=source, dst_ref=sink, send_sem=send_sem, recv_sem=recv_sem, device_id=target, device_id_type=MESH
        )
        copy.start()
        return copy

    sent, local = [], []
    from_z, from_a, from_b, from_d, from_mate, whole = [], [], [], [], [], []
    for k in range(count):
        for i, there in enumerate(others):
            copy = send(shards[k].at[rep], outs[k].at[grp, rep], z_send.at[k, i], z_recv.at[k, i], (rep, 2 * there + core))
            from_z.append(copy)
            sent.append(copy)
    for k in range(count):
        copy = send(shards[k], outs[k].at[grp], s_send.at[k], s_recv.at[k], (rep, mate))
        sent.append(copy)
        whole.append(copy)
        mine = pltpu.make_async_copy(shards[k], outs[k].at[grp], own_sem.at[k])
        mine.start()
        local.append(mine)
    sources = [2 * ((z + 4 - step) % 4) + core for step in (1, 2, 3)]
    for k in range(count):
        for i, origin in enumerate(sources):
            from_z[3 * k + i].wait_recv()
            piece = outs[k].at[origin, rep]
            copy = send(piece, piece, a_send.at[k, i], a_recv.at[k, i], (at_a, grp))
            from_a.append(copy)
            sent.append(copy)
            copy = send(piece, piece, b_send.at[k, i], b_recv.at[k, i], (at_b, grp))
            from_b.append(copy)
            sent.append(copy)
            copy = send(piece, piece, c_send.at[k, 0, i], c_recv.at[k, 0, i], (rep, mate))
            from_mate.append(copy)
            sent.append(copy)
    for k in range(count):
        for i, origin in enumerate(sources):
            from_a[3 * k + i].wait_recv()
            piece = outs[k].at[origin, at_a]
            copy = send(piece, piece, d_send.at[k, i], d_recv.at[k, i], (at_b, grp))
            from_d.append(copy)
            sent.append(copy)
            copy = send(piece, piece, c_send.at[k, 1, i], c_recv.at[k, 1, i], (rep, mate))
            from_mate.append(copy)
            sent.append(copy)
            from_b[3 * k + i].wait_recv()
            piece = outs[k].at[origin, at_b]
            copy = send(piece, piece, c_send.at[k, 2, i], c_recv.at[k, 2, i], (rep, mate))
            from_mate.append(copy)
            sent.append(copy)
    for k in range(count):
        for i, origin in enumerate(sources):
            from_d[3 * k + i].wait_recv()
            piece = outs[k].at[origin, at_d]
            copy = send(piece, piece, c_send.at[k, 3, i], c_recv.at[k, 3, i], (rep, mate))
            from_mate.append(copy)
            sent.append(copy)
    for copy in whole + from_mate:
        copy.wait_recv()
    for copy in sent:
        copy.wait_send()
    for copy in local:
        copy.wait()


def gather_dense(shards, collective_id):
    count = len(shards)
    views = [shard.reshape(4, shard.shape[0] // 4, shard.shape[1]) for shard in shards]
    dma = pltpu.SemaphoreType.DMA
    moved = sum(view.size * 2 for view in views)
    outs = pl.pallas_call(
        functools.partial(gather_kernel, count),
        out_shape=[jax.ShapeDtypeStruct((8,) + view.shape, view.dtype) for view in views],
        in_specs=[pl.BlockSpec(memory_space=pltpu.VMEM)] * count,
        out_specs=[pl.BlockSpec(memory_space=pl.ANY)] * count,
        scratch_shapes=[dma((count,))] + [dma((count, 3))] * 8 + [dma((count, 4, 3))] * 2 + [dma((count,))] * 2,
        compiler_params=pltpu.CompilerParams(collective_id=collective_id, has_side_effects=True),
        cost_estimate=pl.CostEstimate(flops=0, bytes_accessed=16 * moved, transcendentals=0),
        name="gather_dense",
    )(*views)
    return [out.reshape(8 * shard.shape[0], shard.shape[1]) for out, shard in zip(outs, shards)]


ROW_TILE = 1280
FEATURE_TILE = 512


def transposed_product(left_side, right_side):
    return lax.dot_general(
        left_side, right_side, (((1,), (1,)), ((), ())), preferred_element_type=F32
    )


def expert_forward_kernel(at, rows, grads_t, weight, *refs):
    act, slope, share, total = refs[-4:]
    for tile in range(rows.shape[0] // ROW_TILE):
        span = pl.ds(tile * ROW_TILE, ROW_TILE)
        value, turn = gelu_pair(dense_product(rows[span, :], weight[...]))
        value = value.astype(BF16)
        act[span, :] = value
        slope[span, :] = turn.astype(BF16)
        part = dense_product(grads_t[:, span], value)
        if tile == 0:
            total[...] = part
        else:
            total[...] += part
    share[...] = total[...].T.astype(BF16)


def expert_forward(at, rows, grads_t, weight, first, count, held):
    slots, width = rows.shape
    units = weight.shape[2]
    base = first // FEATURE_TILE
    whole = pl.BlockSpec(rows.shape, lambda i, at: (0, 0), pipeline_mode=pl.Buffered(1))
    whole_t = pl.BlockSpec(grads_t.shape, lambda i, at: (0, 0), pipeline_mode=pl.Buffered(1))
    side = pl.BlockSpec((slots, FEATURE_TILE), lambda i, at: (0, base + i))
    return pl.pallas_call(
        expert_forward_kernel,
        out_shape=[
            jax.ShapeDtypeStruct((slots, units), BF16),
            jax.ShapeDtypeStruct((slots, units), BF16),
            jax.ShapeDtypeStruct((count, grads_t.shape[0]), BF16),
        ],
        grid_spec=pltpu.PrefetchScalarGridSpec(
            num_scalar_prefetch=1,
            grid=(count // FEATURE_TILE,),
            in_specs=[
                whole,
                whole_t,
                pl.BlockSpec((None, width, FEATURE_TILE), lambda i, at: (at[0], 0, base + i)),
            ]
            + [pl.BlockSpec(memory_space=pl.ANY)] * len(held),
            out_specs=[
                side,
                side,
                pl.BlockSpec((FEATURE_TILE, grads_t.shape[0]), lambda i, at: (i, 0)),
            ],
            scratch_shapes=[pltpu.VMEM((grads_t.shape[0], FEATURE_TILE), F32)],
        ),
        input_output_aliases={4 + k: k for k in range(len(held))},
        compiler_params=pltpu.CompilerParams(vmem_limit_bytes=60 << 20),
        cost_estimate=pl.CostEstimate(
            flops=4 * slots * width * count,
            bytes_accessed=4 * slots * width + 4 * slots * count + 4 * width * count,
            transcendentals=2 * slots * count,
        ),
        name="expert_forward",
    )(at, rows, grads_t, weight, *held)


def output_gradient_kernel(grads_t, act, share):
    share[...] = dense_product(grads_t[...], act[...]).T.astype(BF16)


def output_gradient(grads_t, act, first, count):
    columns, slots = grads_t.shape
    base = first // FEATURE_TILE
    return pl.pallas_call(
        output_gradient_kernel,
        out_shape=jax.ShapeDtypeStruct((count, columns), BF16),
        grid=(count // FEATURE_TILE,),
        in_specs=[
            pl.BlockSpec(grads_t.shape, lambda i: (0, 0), pipeline_mode=pl.Buffered(1)),
            pl.BlockSpec((slots, FEATURE_TILE), lambda i: (0, base + i)),
        ],
        out_specs=pl.BlockSpec((FEATURE_TILE, columns), lambda i: (i, 0)),
        compiler_params=pltpu.CompilerParams(vmem_limit_bytes=60 << 20),
        cost_estimate=pl.CostEstimate(
            flops=2 * slots * columns * count,
            bytes_accessed=2 * slots * columns + 2 * slots * count + 2 * columns * count,
            transcendentals=0,
        ),
        name="output_gradient",
    )(grads_t, act)


def expert_backward_kernel(
    at, grads, weight_in, weight_out, act, slope, inner, made, sent, made_sum, sent_sum
):
    step = pl.program_id(0)

    @pl.when(step == 0)
    def _():
        made_sum[...] = jnp.zeros_like(made_sum)
        sent_sum[...] = jnp.zeros_like(sent_sum)

    for tile in range(grads.shape[0] // ROW_TILE):
        span = pl.ds(tile * ROW_TILE, ROW_TILE)
        value = transposed_product(grads[span, :], weight_out[...]) * slope[span, :].astype(F32)
        value = value.astype(BF16)
        inner[span, :] = value
        sent_sum[span, :] += transposed_product(value, weight_in[...])
        made_sum[span, :] += dense_product(act[span, :], weight_out[...])

    @pl.when(step == pl.num_programs(0) - 1)
    def _():
        made[...] = made_sum[...].astype(BF16)
        sent[...] = sent_sum[...].astype(BF16)


def expert_backward(at, grads, weight_in, weight_out, act, slope):
    slots, width = grads.shape
    units = weight_in.shape[2]
    whole = pl.BlockSpec(grads.shape, lambda i, at: (0, 0), pipeline_mode=pl.Buffered(1))
    side = pl.BlockSpec((slots, FEATURE_TILE), lambda i, at: (0, i))
    return pl.pallas_call(
        expert_backward_kernel,
        out_shape=[
            jax.ShapeDtypeStruct((slots, units), BF16),
            jax.ShapeDtypeStruct((slots, width), BF16),
            jax.ShapeDtypeStruct((slots, width), BF16),
        ],
        grid_spec=pltpu.PrefetchScalarGridSpec(
            num_scalar_prefetch=1,
            grid=(units // FEATURE_TILE,),
            in_specs=[
                whole,
                pl.BlockSpec((None, width, FEATURE_TILE), lambda i, at: (at[0], 0, i)),
                pl.BlockSpec((None, FEATURE_TILE, width), lambda i, at: (at[0], i, 0)),
                side,
                side,
            ],
            out_specs=[side, whole, whole],
            scratch_shapes=[pltpu.VMEM((slots, width), F32)] * 2,
        ),
        compiler_params=pltpu.CompilerParams(vmem_limit_bytes=63 << 20),
        cost_estimate=pl.CostEstimate(
            flops=6 * slots * width * units,
            bytes_accessed=6 * slots * width + 6 * slots * units + 4 * width * units,
            transcendentals=0,
        ),
        name="expert_backward",
    )(at, grads, weight_in, weight_out, act, slope)


def expert_gradient_kernel(rows_t, inner, top, bottom):
    total = dense_product(rows_t[...], inner[...])
    half = total.shape[0] // 2
    top[...] = total[:half, :].astype(BF16)
    bottom[...] = total[half:, :].astype(BF16)


def expert_gradient(rows_t, inner):
    width, slots = rows_t.shape
    units = inner.shape[1]
    half = pl.BlockSpec((width // 2, FEATURE_TILE), lambda i: (0, i))
    return pl.pallas_call(
        expert_gradient_kernel,
        out_shape=[jax.ShapeDtypeStruct((width // 2, units), BF16)] * 2,
        grid=(units // FEATURE_TILE,),
        in_specs=[
            pl.BlockSpec(rows_t.shape, lambda i: (0, 0), pipeline_mode=pl.Buffered(1)),
            pl.BlockSpec((slots, FEATURE_TILE), lambda i: (0, i)),
        ],
        out_specs=[half, half],
        compiler_params=pltpu.CompilerParams(vmem_limit_bytes=60 << 20),
        cost_estimate=pl.CostEstimate(
            flops=2 * slots * width * units,
            bytes_accessed=2 * slots * width + 2 * slots * units + 2 * width * units,
            transcendentals=0,
        ),
        name="expert_gradient",
    )(rows_t, inner)


def scatter_kernel(grad, out, mated, halves, planar, quarters, lined, done, sems):
    m_send, m_recv, p_send, p_recv, l_send, l_recv, d_send, d_recv = sems
    rep, grp = lax.axis_index("rep"), lax.axis_index("grp")
    y, x = rep // 2, rep % 2
    z, core = grp // 2, grp % 2
    plane = [2 * y + 1 - x, 2 * (1 - y) + x, 2 * (1 - y) + 1 - x]
    line = [(z + step) % 4 for step in (1, 2, 3)]
    mate = (rep, 2 * z + 1 - core)

    barrier = pltpu.get_barrier_semaphore()
    for target in [mate] + [(there, grp) for there in plane] + [(rep, 2 * k + core) for k in line]:
        pl.semaphore_signal(barrier, inc=1, device_id=target, device_id_type=MESH)
    pl.semaphore_wait(barrier, 7)

    def send(source, sink, send_sem, recv_sem, target):
        copy = pltpu.make_async_remote_copy(
            src_ref=source,
            dst_ref=sink,
            send_sem=send_sem,
            recv_sem=recv_sem,
            device_id=target,
            device_id_type=MESH,
        )
        copy.start()
        return copy

    to_mate = [
        send(grad.at[k, 1 - core], mated.at[k], m_send.at[k], m_recv.at[k], mate) for k in range(4)
    ]
    to_plane = []
    for k in range(4):
        to_mate[k].wait_recv()
        for q in range(4):
            total = grad[k, core, q].astype(F32) + mated[k, q].astype(F32)
            halves[k, q] = total.astype(BF16)
        to_plane.append(
            [
                send(
                    halves.at[k, there],
                    planar.at[i, k],
                    p_send.at[i, k],
                    p_recv.at[i, k],
                    (there, grp),
                )
                for i, there in enumerate(plane)
            ]
        )
    to_line = []
    for k in range(4):
        for copy in to_plane[k]:
            copy.wait_recv()
        total = halves[k, rep].astype(F32)
        for i in range(3):
            total += planar[i, k].astype(F32)
        quarters[k] = total.astype(BF16)
    for i, there in enumerate(line):
        to_line.append(
            send(
                quarters.at[there],
                lined.at[i],
                l_send.at[i],
                l_recv.at[i],
                (rep, 2 * there + core),
            )
        )
    total = quarters[z].astype(F32)
    for i in range(3):
        to_line[i].wait_recv()
        total += lined[i].astype(F32)
    done[rep] = total.astype(BF16)
    to_all = [
        send(done.at[rep], done.at[rep], d_send.at[i], d_recv.at[i], (there, grp))
        for i, there in enumerate(plane)
    ]
    for copy in to_all:
        copy.wait_recv()
    for q in range(4):
        out[q] = done[q].astype(F32)
    for copy in to_mate + [copy for row in to_plane for copy in row] + to_line + to_all:
        copy.wait_send()


def scatter_dense(grad, collective_id):
    rows, columns = grad.shape[0] // 32, grad.shape[1]
    dma = pltpu.SemaphoreType.DMA
    block = (rows, columns)

    def kernel(grad, out, mated, halves, planar, quarters, lined, done, *sems):
        scatter_kernel(grad, out, mated, halves, planar, quarters, lined, done, sems)

    out = pl.pallas_call(
        kernel,
        out_shape=jax.ShapeDtypeStruct((4,) + block, F32),
        in_specs=[pl.BlockSpec(memory_space=pltpu.VMEM)],
        out_specs=pl.BlockSpec(memory_space=pltpu.VMEM),
        scratch_shapes=[
            pltpu.VMEM((4, 4) + block, BF16),
            pltpu.VMEM((4, 4) + block, BF16),
            pltpu.VMEM((3, 4) + block, BF16),
            pltpu.VMEM((4,) + block, BF16),
            pltpu.VMEM((3,) + block, BF16),
            pltpu.VMEM((4,) + block, BF16),
        ]
        + [dma((4,))] * 2
        + [dma((3, 4))] * 2
        + [dma((3,))] * 4,
        compiler_params=pltpu.CompilerParams(
            collective_id=collective_id, has_side_effects=True, vmem_limit_bytes=60 << 20
        ),
        cost_estimate=pl.CostEstimate(flops=0, bytes_accessed=64 * rows * columns, transcendentals=0),
        name="scatter_dense",
    )(grad.reshape((4, 2, 4) + block))
    return out.reshape(4 * rows, columns)


def place_kernel(at, piece, *refs):
    refs[-1][...] = piece[...].astype(F32)


def place(held, piece, expert, count, shape, row, column):
    rows, columns = piece.shape
    tile = rows // 3 if columns > 1024 else rows // 2
    in_specs = [pl.BlockSpec((tile, columns), lambda i, at: (i, 0))]
    operands = [expert.reshape(1), piece]
    if held is not None:
        in_specs.append(pl.BlockSpec(memory_space=pl.ANY))
        operands.append(held)
    return pl.pallas_call(
        place_kernel,
        out_shape=jax.ShapeDtypeStruct((count,) + shape, F32),
        grid_spec=pltpu.PrefetchScalarGridSpec(
            num_scalar_prefetch=1,
            grid=(rows // tile,),
            in_specs=in_specs,
            out_specs=pl.BlockSpec(
                (None, tile, columns), lambda i, at: (at[0], row // tile + i, column // columns)
            ),
        ),
        input_output_aliases={2: 0} if held is not None else {},
        cost_estimate=pl.CostEstimate(
            flops=0, bytes_accessed=6 * rows * columns, transcendentals=0
        ),
        name="place",
    )(*operands)


def complete(rep_at, pieces, shape):
    over_x, over_y = [(i, i ^ 1) for i in range(4)], [(i, i ^ 2) for i in range(4)]
    near = []
    for piece, _, _ in pieces:
        near.append((swap(piece, over_x), swap(piece, over_y)))
    far = [swap(near[k][k % 2], over_x if k % 2 else over_y) for k in range(len(pieces))]
    order = [(k, 0, piece) for k, (piece, _, _) in enumerate(pieces)]
    order += [(k, 1 + i, near[k][i]) for k in range(len(pieces)) for i in range(2)]
    order += [(k, 3, piece) for k, piece in enumerate(far)]
    held = None
    for k, away, piece in order:
        held = place(held, piece, rep_at ^ away, 4, shape, pieces[k][1], pieces[k][2])
    return held


def swap(operand, axis_pairs):
    return lax.ppermute(operand, "rep", axis_pairs)


def local(
    n_rep,
    n_grp,
    block_in,
    out_grad,
    routes,
    ln1_gain,
    ln1_bias,
    w_qkv,
    w_proj,
    ln2_gain,
    ln2_bias,
    w_fc1,
    w_fc2,
    ln3_gain,
    ln3_bias,
    w_router,
    expert_in,
    expert_out,
):
    bf16, f32 = jnp.bfloat16, jnp.float32
    scaling = HEAD_DIM ** (-0.5)
    tok_rows, width = block_in.shape
    held = expert_in.shape[0]
    spread = n_rep if held % n_rep == 0 else 1
    own = held // spread
    axes = ("rep", "grp") if spread > 1 else ("grp",)
    peers = spread * n_grp
    rep_at = lax.axis_index("rep")

    def gather(shard):
        return lax.all_gather(shard, "grp", axis=0, tiled=True)

    vectors = jnp.stack([ln1_gain, ln1_bias, ln2_gain, ln2_bias, ln3_gain, ln3_bias], axis=1)
    narrow = jnp.concatenate([w_router, vectors], axis=1)
    if n_rep == 4 and n_grp == 8:
        lanes = 128 - narrow.shape[1]
        joint = jnp.concatenate([w_qkv, w_proj, jnp.pad(narrow, ((0, 0), (0, lanes)))], axis=1)
        joint, full_fc1, full_fc2 = gather_dense([joint, w_fc1, w_fc2], 0)
        full_qkv = joint[:, : 3 * width]
        full_proj = joint[:, 3 * width : 4 * width]
        narrow = joint[:, 4 * width :]
    else:
        full_qkv, full_proj, full_fc1, full_fc2, narrow = map(
            gather, (w_qkv, w_proj, w_fc1, w_fc2, narrow)
        )
    full_router, small = narrow[:, :EXPERTS], narrow[:, EXPERTS : EXPERTS + 6]
    small = small.astype(f32).T
    gain_first, shift_first, gain_second, shift_second, gain_third, shift_third = small

    expert_ids = lax.iota(jnp.int32, EXPERTS)
    route_picks = routes[:, :, None] == expert_ids[None, None, :]
    hits = jnp.any(route_picks, axis=1)
    earlier = (
        lax.broadcasted_iota(jnp.int32, (tok_rows, tok_rows), 1)
        < lax.broadcasted_iota(jnp.int32, (tok_rows, tok_rows), 0)
    ).astype(bf16)
    ranks = dense_product(earlier, hits.astype(bf16)).astype(jnp.int32)
    rank = jnp.sum(jnp.where(route_picks, ranks[:, None, :], 0), axis=-1)
    group_of, within = routes // held, routes % held
    place = ((within // own) * n_grp + group_of) * own + within % own
    slot = place * SLOTS + rank
    slot_ids = lax.iota(jnp.int32, EXPERTS * SLOTS)
    pick_first = (slot[:, 0][:, None] == slot_ids[None, :]).astype(bf16)
    pick_second = (slot[:, 1][:, None] == slot_ids[None, :]).astype(bf16)
    pick_both = pick_first + pick_second

    def exchange(rows):
        return lax.all_to_all(rows, axes, split_axis=0, concat_axis=0, tiled=True)

    def to_experts(rows):
        rows = exchange(rows.reshape((peers, own, SLOTS) + rows.shape[1:]))
        return jnp.moveaxis(rows, 1, 0).reshape((own, peers * SLOTS) + rows.shape[3:])

    def to_tokens(rows):
        rows = jnp.moveaxis(rows.reshape((own, peers, SLOTS) + rows.shape[2:]), 1, 0)
        return exchange(rows).reshape((EXPERTS * SLOTS,) + rows.shape[3:])

    cut = width // 2
    grad_rows = rows_product(pick_both, out_grad).astype(bf16)
    grad_left = to_experts(grad_rows[:, :cut])
    grad_right = to_experts(grad_rows[:, cut:])

    stream = block_in.astype(f32)
    normed_one = layer_norm(stream, gain_first, shift_first).astype(bf16)
    packed = dense_product(normed_one, full_qkv).astype(bf16)
    attn_mixed = attend(packed, scaling)
    after_attn = stream + dense_product(attn_mixed, full_proj)
    normed_two = layer_norm(after_attn, gain_second, shift_second).astype(bf16)
    hidden, hidden_slope = gelu_pair(dense_product(normed_two, full_fc1))
    hidden, hidden_slope = hidden.astype(bf16), hidden_slope.astype(bf16)
    second = after_attn + dense_product(hidden, full_fc2)
    normed_three = layer_norm(second, gain_third, shift_third).astype(bf16)
    arrived = to_experts(rows_product(pick_both, normed_three).astype(bf16))

    logits = dense_product(normed_three, full_router)
    chosen = jnp.sum(jnp.where(route_picks, logits[:, None, :], 0.0), axis=-1)
    chosen_exp = jnp.exp(chosen - jnp.max(chosen, axis=-1, keepdims=True))
    gate_probs = chosen_exp / jnp.sum(chosen_exp, axis=-1, keepdims=True)
    hit_first = slot[:, 0][:, None] == slot_ids[None, :]
    hit_second = slot[:, 1][:, None] == slot_ids[None, :]
    gate_rows = jnp.sum(
        jnp.where(hit_first, gate_probs[:, 0][:, None], 0.0)
        + jnp.where(hit_second, gate_probs[:, 1][:, None], 0.0),
        axis=0,
    )
    gate_slots = to_experts(gate_rows)

    half = expert_in.shape[2] // 2
    made, sent_back, out_parts, in_parts, gate_parts = [], [], [], [], []
    for j in range(own):
        at = (rep_at * own + j if spread > 1 else jnp.int32(j)).reshape(1).astype(jnp.int32)
        rows, gates = arrived[j], gate_slots[j]
        left_t = lax.optimization_barrier(grad_left[j].T)
        left_t = (gates[None, :] * left_t.astype(f32)).astype(bf16)
        right_t = (gates[None, :] * grad_right[j].T.astype(f32)).astype(bf16)
        grad_float = jnp.concatenate([grad_left[j], grad_right[j]], axis=1).astype(f32)
        grads = (gates[:, None] * grad_float).astype(bf16)
        act, slope, left_top = expert_forward(at, rows, left_t, expert_in, 0, half, ())
        act, slope, left_bottom = expert_forward(
            at, rows, left_t, expert_in, half, half, (act, slope)
        )
        right_top = output_gradient(right_t, act, 0, half)
        right_bottom = output_gradient(right_t, act, half, half)
        inner, result, back = expert_backward(at, grads, expert_in, expert_out, act, slope)
        in_top, in_bottom = expert_gradient(rows.T, inner)
        out_parts.append(
            [(left_top, 0, 0), (left_bottom, half, 0), (right_top, 0, cut), (right_bottom, half, cut)]
        )
        in_parts.append([(in_top, 0, 0), (in_bottom, cut, 0)])
        made.append(result)
        sent_back.append(back)
        gate_parts.append(jnp.sum(grad_float * result.astype(f32), axis=-1))
    produced, grad_sent = jnp.stack(made), jnp.stack(sent_back)
    gate_grads = to_tokens(jnp.stack(gate_parts))
    grad_returned = to_tokens(grad_sent)
    returned = to_tokens(produced)

    def joined(pieces):
        columns = {}
        for piece, _, column in pieces:
            columns.setdefault(column, []).append(piece)
        return jnp.concatenate([jnp.concatenate(c) for c in columns.values()], axis=1)

    def finish(parts, shape):
        if spread == 4 and own == 1:
            return complete(rep_at, parts[0], shape)
        finished = jnp.stack([joined(pieces) for pieces in parts])
        if spread > 1:
            return lax.all_gather(finished, "rep", axis=0, tiled=True).astype(f32)
        return lax.psum(finished, "rep").astype(f32)

    full_grad_out = finish(out_parts, expert_out.shape[1:])
    full_grad_in = finish(in_parts, expert_in.shape[1:])

    first_rows = dense_product(pick_first, returned)
    second_rows = dense_product(pick_second, returned)
    block_out = second + (gate_probs[:, :1] * first_rows + gate_probs[:, 1:] * second_rows)
    top_grad = out_grad.astype(f32)
    grad_gate = jnp.stack(
        [
            jnp.sum(jnp.where(hit_first, gate_grads[None, :], 0.0), axis=1),
            jnp.sum(jnp.where(hit_second, gate_grads[None, :], 0.0), axis=1),
        ],
        axis=1,
    )
    grad_chosen = gate_probs * (grad_gate - jnp.sum(gate_probs * grad_gate, axis=-1, keepdims=True))
    grad_logits = jnp.sum(jnp.where(route_picks, grad_chosen[:, :, None], 0.0), axis=1)
    router_float = full_router.astype(f32)
    grad_normed_three = dense_product(pick_both, grad_returned) + jnp.dot(
        grad_logits, router_float.T, precision=lax.Precision.HIGHEST, preferred_element_type=f32
    )
    grad_router = jnp.dot(
        normed_three.astype(f32).T,
        grad_logits,
        precision=lax.Precision.HIGHEST,
        preferred_element_type=f32,
    )
    grad_second, grad_gain_three, grad_shift_three = norm_back(
        second, gain_third, shift_third, grad_normed_three
    )
    grad_second = top_grad + grad_second

    def shares(partial):
        return lax.psum_scatter(partial.astype(bf16), "grp", scatter_dimension=0, tiled=True)

    grad_branch = grad_second.astype(bf16)
    grad_fc2 = rows_product(hidden, grad_branch).astype(bf16)
    share_fc2 = shares(grad_fc2)
    grad_before = (column_product(grad_branch, full_fc2) * hidden_slope.astype(f32)).astype(bf16)
    grad_fc1 = rows_product(normed_two, grad_before).astype(bf16)
    share_fc1 = shares(grad_fc1)
    grad_after, grad_gain_two, grad_shift_two = norm_back(
        after_attn, gain_second, shift_second, column_product(grad_before, full_fc1)
    )
    grad_after = grad_second + grad_after
    grad_attend = grad_after.astype(bf16)
    grad_proj = rows_product(attn_mixed, grad_attend).astype(bf16)
    grad_mixed = column_product(grad_attend, full_proj).astype(bf16)
    grad_parts = attend_back(packed, grad_mixed, scaling)
    grad_normed_one = sum(
        column_product(part, full_qkv[:, k * width : (k + 1) * width])
        for k, part in enumerate(grad_parts)
    )
    grad_stream, grad_gain_one, grad_shift_one = norm_back(
        stream, gain_first, shift_first, grad_normed_one
    )
    grad_qkv = [rows_product(normed_one, part).astype(bf16) for part in grad_parts]
    grad_in = grad_after + grad_stream
    vectors = jnp.stack(
        [
            grad_gain_one,
            grad_shift_one,
            grad_gain_two,
            grad_shift_two,
            grad_gain_three,
            grad_shift_three,
        ],
        axis=1,
    )
    narrow = jnp.concatenate([grad_router, vectors], axis=1).astype(bf16)
    if n_rep == 4 and n_grp == 8:
        lanes = 128 - narrow.shape[1]
        joint = jnp.concatenate(
            [*grad_qkv, grad_proj, jnp.pad(narrow, ((0, 0), (0, lanes)))], axis=1
        )
        joint = scatter_dense(joint, 1)
        total_qkv = joint[:, : 3 * width]
        total_proj = joint[:, 3 * width : 4 * width]
        total_small = joint[:, 4 * width :]
    else:
        total_qkv, total_proj, total_small = (
            lax.psum(shares(part), "rep").astype(f32) for part in (jnp.concatenate(grad_qkv, axis=1), grad_proj, narrow)
        )

    def over_replicas(share):
        if n_rep != 4:
            return lax.psum(share, "rep").astype(f32)
        others = [swap(share, [(i, i ^ away) for i in range(4)]) for away in (1, 2, 3)]
        return sum(part.astype(f32) for part in [share] + others)

    total_fc1 = over_replicas(share_fc1)
    total_fc2 = over_replicas(share_fc2)
    return (
        block_out,
        grad_in,
        total_small[:, EXPERTS],
        total_small[:, EXPERTS + 1],
        total_qkv,
        total_proj,
        total_small[:, EXPERTS + 2],
        total_small[:, EXPERTS + 3],
        total_fc1,
        total_fc2,
        total_small[:, EXPERTS + 4],
        total_small[:, EXPERTS + 5],
        total_small[:, :EXPERTS],
        full_grad_in,
        full_grad_out,
    )


def solution(mesh):
    return jax.shard_map(
        functools.partial(local, mesh.shape["rep"], mesh.shape["grp"]),
        mesh=mesh,
        in_specs=(
            P(("rep", "grp"), None),
            P(("rep", "grp"), None),
            P(("rep", "grp"), None),
            P("grp"),
            P("grp"),
            P("grp", None),
            P("grp", None),
            P("grp"),
            P("grp"),
            P("grp", None),
            P("grp", None),
            P("grp"),
            P("grp"),
            P("grp", None),
            P("grp", None, None),
            P("grp", None, None),
        ),
        out_specs=(
            P(("rep", "grp"), None),
            P(("rep", "grp"), None),
            P("grp"),
            P("grp"),
            P("grp", None),
            P("grp", None),
            P("grp"),
            P("grp"),
            P("grp", None),
            P("grp", None),
            P("grp"),
            P("grp"),
            P("grp", None),
            P("grp", None, None),
            P("grp", None, None),
        ),
        check_vma=False,
    )
```
